256 devices in a mesh: section: 8 (over y, x_hi), dp: 32 (over z, x_lo, core).
Axes of the slice: x: 4 (x_hi: 2, x_lo: 2; x = x_hi * 2 + x_lo), y: 4, z: 8, core: 2. Of those that a mesh axis runs over, the one named last changes fastest.
Arguments:
- block_inputs: bfloat16 [8, 4, 2048, 2048], P('section', None, 'dp'), may hold values from -6 to 6
- mixed_inputs: bfloat16 [8, 4, 2048, 2048], P('section', None, 'dp'), may hold values from -6 to 6
- token_ids: int32 [4, 2048], P(None, 'dp'), may hold values from 0 to 2047
- target_ids: int32 [4, 2048], P(None, 'dp'), may hold values from 0 to 2047
- final_gain: float32 [2048], replicated, may hold values from 0.5 to 1.5
- out_weight: bfloat16 [8, 2048, 2048], P('section'), may hold values from -0.046875 to 0.046875
- head_weight: bfloat16 [2048, 2048], P('section'), may hold values from -0.375 to 0.375
- out_master: float32 [8, 2048, 2048], P('section', 'dp'), may hold values from -0.125 to 0.125
- out_first: float32 [8, 2048, 2048], P('section', 'dp'), may hold values from -2.5 to 2.5
- out_second: float32 [8, 2048, 2048], P('section', 'dp'), may hold values from 4 to 80
- head_master: float32 [2048, 2048], P(('section', 'dp')), may hold values from -0.125 to 0.125
- head_first: float32 [2048, 2048], P(('section', 'dp')), may hold values from -1.5 to 1.5
- head_second: float32 [2048, 2048], P(('section', 'dp')), may hold values from 1.2 to 24
- embed_master: float32 [2048, 2048], P(('section', 'dp')), may hold values from -0.125 to 0.125
- embed_first: float32 [2048, 2048], P(('section', 'dp')), may hold values from -0.125 to 0.125
- embed_second: float32 [2048, 2048], P(('section', 'dp')), may hold values from 0.009765625 to 0.1953125
Outputs:
- out_master_next: float32 [8, 2048, 2048], P('section', 'dp')
- out_first_next: float32 [8, 2048, 2048], P('section', 'dp')
- out_second_next: float32 [8, 2048, 2048], P('section', 'dp')
- head_master_next: float32 [2048, 2048], P(('section', 'dp'))
- head_first_next: float32 [2048, 2048], P(('section', 'dp'))
- head_second_next: float32 [2048, 2048], P(('section', 'dp'))
- embed_master_next: float32 [2048, 2048], P(('section', 'dp'))
- embed_first_next: float32 [2048, 2048], P(('section', 'dp'))
- embed_second_next: float32 [2048, 2048], P(('section', 'dp'))
The draws below stay inside these ranges and needn't reach their ends.
Inputs may be any that keep to these rules, and one draw needn't show every extreme that they name: `token_ids`: every token id lies in 0 to 2047. `target_ids`: every target id lies in 0 to 2047.
All inputs are finite; a program needn't handle non-finite values.
Results may differ from the reference program's by a relative error of at most 0.00155.
Values may be sent and summed in bfloat16 or wider, within the bound.
A program may use at most 128 MiB of HBM per device.

```python
import math
import jax
import jax.numpy as jnp
import numpy as np
from jax import lax

D = 2048
VOCAB = 2048
MICRO = 4
TOKENS_MB = 2048
N_SECTION = 8


def with_ends(entries, key, least, largest):
    longest = entries.shape.index(max(entries.shape))
    spots = []
    for shift in (0, 1):
        where = [jax.random.randint(jax.random.fold_in(key, axis), (), 0, length) for axis, length in enumerate(entries.shape)]
        where[longest] = (where[longest] + shift) % entries.shape[longest]
        spots.append(tuple(where))
    return entries.at[spots[0]].set(least).at[spots[1]].set(largest)


def level_of(key, shape, shards, least, top_value):
    level = 1.0
    for position, shards_of in shards:
        steps = jax.random.uniform(jax.random.fold_in(jax.random.fold_in(key, 6), position), (shards_of,), jnp.float32, least / len(shards), top_value / len(shards))
        level = level * jnp.repeat(jnp.exp(steps), shape[position] // shards_of).reshape((-1,) + (1,) * (len(shape) - 1 - position))
    return level


def rank_table(amount, skew):
    portions = [(1 << 20) // math.isqrt(grade ** skew) + 1 for grade in range(1, amount + 1)]
    deviation = 1 + sum(portions) // (1 << 30)
    return np.cumsum(np.array([max(1, weight // deviation) for weight in portions]))


def ranked_ids(own_key, shape, number_of, slope):
    grid = rank_table(number_of, slope)
    ticket = jax.random.randint(jax.random.fold_in(own_key, 1), shape, 0, int(grid[number_of - 1]))
    rank = jnp.searchsorted(jnp.asarray(grid, jnp.int32), ticket, side="right")
    return jax.random.permutation(jax.random.fold_in(own_key, 2), number_of)[rank].astype(jnp.int32)


def centred(stream_key, shape, spread, bound, pieces=(), dtype=jnp.bfloat16):
    result = spread * jax.random.normal(stream_key, shape, jnp.float32)
    if pieces:
        result = result * level_of(stream_key, shape, pieces, -0.22, 0.18)
    return jnp.clip(result, -bound, bound).astype(dtype)


def setup_inputs(seed: int = 0) -> dict:
    arg_keys = jax.random.split(jax.random.key(seed), 17)
    return {
        "block_inputs": centred(arg_keys[0], (N_SECTION, MICRO, TOKENS_MB, D), 1.0, 6.0, ((0, 8), (2, 32))),
        "mixed_inputs": centred(arg_keys[1], (N_SECTION, MICRO, TOKENS_MB, D), 1.0, 6.0, ((0, 8), (2, 32))),
        "token_ids": with_ends(ranked_ids(arg_keys[2], (MICRO, TOKENS_MB), VOCAB, 2), jax.random.fold_in(arg_keys[2], 3), 0, VOCAB - 1).astype(jnp.int32),
        "target_ids": with_ends(ranked_ids(arg_keys[3], (MICRO, TOKENS_MB), VOCAB, 2), jax.random.fold_in(arg_keys[3], 3), 0, VOCAB - 1).astype(jnp.int32),
        "final_gain": jnp.clip(1.0 + 0.1 * jax.random.normal(arg_keys[4], (D,), jnp.float32), 0.5, 1.5),
        "out_weight": centred(arg_keys[5], (N_SECTION, D, D), (D * N_SECTION) ** -0.5, 0.046875, ((0, 8),)),
        "head_weight": centred(arg_keys[6], (VOCAB, D), (3 * D ** -0.5), 0.375, ((0, 8),)),
        "out_master": centred(arg_keys[7], (N_SECTION, D, D), D ** -0.5, 0.125, ((0, 8), (1, 32)), jnp.float32),
        "out_first": centred(arg_keys[8], (N_SECTION, D, D), (0.2 * (MICRO * TOKENS_MB) ** 0.5 * D ** -0.5), 2.5, ((0, 8), (1, 32)), jnp.float32),
        "out_second": jnp.clip(jnp.exp(math.log(80.0) - 2.9957323 * jax.random.uniform(arg_keys[9], (N_SECTION, D, D), jnp.float32) ** level_of(arg_keys[9], (N_SECTION, D, D), ((0, 8), (1, 32)), -0.2, 0.2)), 4.0, 80.0),
        "head_master": centred(arg_keys[10], (VOCAB, D), D ** -0.5, 0.125, ((0, 256),), jnp.float32),
        "head_first": centred(arg_keys[11], (VOCAB, D), (0.12 * (MICRO * TOKENS_MB) ** 0.5 * VOCAB ** -0.5), 1.5, ((0, 256),), jnp.float32),
        "head_second": jnp.clip(jnp.exp(math.log(24.0) - 2.9957322 * jax.random.uniform(arg_keys[12], (VOCAB, D), jnp.float32) ** level_of(arg_keys[12], (VOCAB, D), ((0, 256),), -0.2, 0.2)), 1.2, 24.0),
        "embed_master": centred(arg_keys[13], (VOCAB, D), D ** -0.5, 0.125, ((0, 256),), jnp.float32),
        "embed_first": centred(arg_keys[14], (VOCAB, D), (0.5 * (MICRO * TOKENS_MB) ** 0.5 * (VOCAB * D) ** -0.5), 0.125, ((0, 256),), jnp.float32),
        "embed_second": jnp.clip(jnp.exp(math.log(0.1953125) - 2.9957323 * jax.random.uniform(arg_keys[15], (VOCAB, D), jnp.float32) ** level_of(arg_keys[15], (VOCAB, D), ((0, 256),), -0.2, 0.2)), 0.009765625, 0.1953125),
    }


norm_eps = 1e-05
beta_first = 0.9
beta_second = 0.95
adam_eps = 1e-05
learning_rate = 0.0003
decay_rate = 0.1

def times_transposed(former, latter):
    return lax.dot_general(former, latter, (((1,), (1,)), ((), ())), preferred_element_type=jnp.float32)

def transposed_times(former, latter):
    return lax.dot_general(former, latter, (((0,), (0,)), ((), ())), preferred_element_type=jnp.float32)

def plain_times(former, latter):
    return jnp.dot(former, latter, preferred_element_type=jnp.float32)

def normalize(values, gain):
    inverse = lax.rsqrt(lax.optimization_barrier(jnp.mean(values * values, axis=-1, keepdims=True)) + norm_eps)
    return (inverse, values * inverse * gain)

def norm_backward(values, inverse, scaled_cotangent):
    unit = values * inverse
    return inverse * (scaled_cotangent - unit * lax.optimization_barrier(jnp.mean(scaled_cotangent * unit, axis=-1, keepdims=True)))

def adam_update(master, first, second, gradient):
    first_next = beta_first * first + (1.0 - beta_first) * gradient
    second_next = beta_second * second + (1.0 - beta_second) * gradient * gradient
    master_next = master - learning_rate * (first_next / (jnp.sqrt(second_next) + adam_eps) + decay_rate * master)
    return (master_next, first_next, second_next)

def reference(block_inputs, mixed_inputs, token_ids, target_ids, final_gain, out_weight, head_weight, out_master, out_first, out_second, head_master, head_first, head_second, embed_master, embed_first, embed_second):
    last = N_SECTION - 1
    count = MICRO * TOKENS_MB
    wide = block_inputs[last].reshape(count, D).astype(jnp.float32)
    final = wide + times_transposed(mixed_inputs[last].reshape(count, D), out_weight[last])
    final_inverse, final_scaled = normalize(final, final_gain)
    last_hidden = final_scaled.astype(jnp.bfloat16)
    logits = times_transposed(last_hidden, head_weight)
    predicted = jax.nn.softmax(logits, axis=-1)
    columns = lax.broadcasted_iota(jnp.int32, (1, VOCAB), 1)
    hits = (target_ids.reshape(-1)[:, None] == columns).astype(jnp.float32)
    logit_cotangent = (predicted - hits).astype(jnp.bfloat16)
    head_gradient = transposed_times(logit_cotangent, last_hidden)
    hidden_cotangent = plain_times(logit_cotangent, head_weight)
    cotangent = norm_backward(final, final_inverse, hidden_cotangent * final_gain).astype(jnp.bfloat16)
    parts = []
    for section in range(N_SECTION):
        parts.append(transposed_times(cotangent, mixed_inputs[section].reshape(count, D)))
    out_gradient = jnp.stack(parts)
    embed_gradient = jax.ops.segment_sum(cotangent.astype(jnp.float32), token_ids.reshape(-1), num_segments=VOCAB)
    out_out = adam_update(out_master, out_first, out_second, out_gradient)
    head_out = adam_update(head_master, head_first, head_second, head_gradient)
    embed_out = adam_update(embed_master, embed_first, embed_second, embed_gradient)
    return (out_out[0], out_out[1], out_out[2], head_out[0], head_out[1], head_out[2], embed_out[0], embed_out[1], embed_out[2])
```

```python
import jax
import jax.numpy as jnp
from jax import lax
from jax.experimental import pallas as pl
from jax.experimental.pallas import tpu as pltpu
from jax.sharding import PartitionSpec as P

norm_eps = 1e-05
beta_first = 0.9
beta_second = 0.95
adam_eps = 1e-05
learning_rate = 0.0003
decay_rate = 0.1
MESH = pl.DeviceIdType.MESH
bf16, f32 = jnp.bfloat16, jnp.float32
SECTIONS, REPLICAS = 8, 32
TOKENS, WIDTH, VOCAB = 256, 2048, 2048
BLOCK = TOKENS // SECTIONS
SLICE = VOCAB // SECTIONS
OWNED = 64
NT = (((1,), (1,)), ((), ()))
TN = (((0,), (0,)), ((), ()))


def dot(a, b, dims):
    return lax.dot_general(a, b, dims, preferred_element_type=f32)


def y_peer(y, k):
    return (y, y + 1 - 2 * (y % 2), (y + 2) % 4, 3 - y)[k]


def flip(value, k):
    return 1 - value if k else value


def kernel(
    wide_hbm, mixed_hbm, head_hbm, weight_hbm, gain, targets, ids,
    out_grad, head_grad, embed_grad,
    mix, hd, wbuf, wide, final, hid, stats, hmine, smine, lg, lcb, hc, cotb,
    gcot, bcot, ghid, bhid, alog, idsb, psum, psend, rs, rs0, tile_e, tile_h, er, hr,
    loc, hs, hrv, fs, fr, ms, mr, ns, nr, ts, tr, ls, lr, gs, gr, cs, cr, is_, ir,
    vs, vr, ws, wr, rss, rsr, es, erv, zs, zr,
):
    section = lax.axis_index("section")
    replica = lax.axis_index("dp")
    y, xh = section // 2, section % 2
    z, xl, c = replica // 4, (replica // 2) % 2, replica % 2
    sigma = 1 - 2 * (z % 2)
    root = section == SECTIONS - 1

    def dev(y_, xh_, z_, xl_, c_):
        return (y_ * 2 + xh_, z_ * 4 + xl_ * 2 + c_)

    def section_peer(j, cross=False):
        ky, kx = j // 2, j % 2
        return dev(y_peer(y, ky), flip(xh, kx), z, flip(xl, kx) if cross else xl, c)

    def member(m):
        kz, kl, kc = m // 4, (m // 2) % 2, m % 2
        return (z + 4 * kz) % 8, flip(xl, kl), flip(c, kc)

    def remote(src, dst, send, recv, device):
        return pltpu.make_async_remote_copy(
            src_ref=src, dst_ref=dst, send_sem=send, recv_sem=recv,
            device_id=device, device_id_type=MESH,
        )

    load_mix = pltpu.make_async_copy(mixed_hbm, mix.at[0], loc.at[0])
    load_head = pltpu.make_async_copy(head_hbm, hd.at[section], loc.at[1])
    load_mix.start()
    load_head.start()
    load_wide = pltpu.make_async_copy(wide_hbm, wide, loc.at[2])

    def load_weight(n):
        return pltpu.make_async_copy(weight_hbm.at[pl.ds(n * 256, 256)], wbuf.at[n], loc.at[4 + n])

    @pl.when(root)
    def _():
        load_wide.start()
        for n in range(8):
            load_weight(n).start()

    barrier = pltpu.get_barrier_semaphore()
    for j in range(1, 8):
        pl.semaphore_signal(barrier, inc=1, device_id=section_peer(j), device_id_type=MESH)
        if j % 2:
            pl.semaphore_signal(barrier, inc=1, device_id=section_peer(j, True), device_id_type=MESH)

    def greet(k, carry):
        pl.semaphore_signal(
            barrier, inc=1, device_id=(section, (replica + k) % REPLICAS), device_id_type=MESH
        )
        return carry

    lax.fori_loop(1, REPLICAS, greet, 0)
    pl.semaphore_wait(barrier, 7 + 4 + REPLICAS - 1)

    half = pl.ds(pl.multiple_of(c * 128, 128), 128)
    load_head.wait()
    head_sends = []
    for j in (2, 6, 1, 4, 3, 7, 5):
        own = hd.at[section, half]
        copy = remote(own, own, hs.at[j], hrv.at[j], section_peer(j, True))
        copy.start()
        head_sends.append(copy)
    load_mix.wait()
    partner = dev(y, xh, z, xl, 1 - c)

    def mix_copy(src, dst, device):
        return remote(mix.at[src], mix.at[dst], ms.at[dst], mr.at[dst], device)

    mix_xl = mix_copy(0, 2, dev(y, xh, z, 1 - xl, c))
    mix_z = mix_copy(0, 4, dev(y, xh, (z + 4) % 8, xl, c))
    mix_diag = mix_copy(4, 6, dev(y, xh, z, 1 - xl, c))
    mix_core = [mix_copy(m, m + 1, partner) for m in (0, 2, 4, 6)]
    mix_z.start()
    mix_xl.start()
    mix_core[0].start()
    own_ids = pltpu.make_async_copy(ids, idsb.at[0], loc.at[3])
    own_ids.start()
    ids_sends = []
    for m in range(1, 8):
        copy = remote(ids, idsb.at[m], is_.at[m], ir.at[m], dev(y, xh, *member(m)))
        copy.start()
        ids_sends.append(copy)

    def hidden_send(j):
        ky, kx = j // 2, j % 2
        peer = section_peer(j)
        rows = pl.ds(pl.multiple_of(peer[0] * BLOCK, BLOCK), BLOCK)
        return (
            remote(hid.at[rows], hmine, ts.at[0, j], tr.at[0], peer),
            remote(stats.at[rows], smine, ts.at[1, j], tr.at[1], peer),
        )

    @pl.when(root)
    def _():
        load_wide.wait()
        for n in range(8):
            load_weight(n).wait()

        def columns(n, carry):
            cols = pl.ds(pl.multiple_of(n * 256, 256), 256)
            final[:, cols] = dot(mix[0], wbuf[n], NT) + wide[:, cols].astype(f32)
            return carry

        lax.fori_loop(0, 8, columns, 0)

        def norm(b, carry):
            rows = pl.ds(pl.multiple_of(b * BLOCK, BLOCK), BLOCK)
            values = final[rows, :]
            inverse = lax.rsqrt(jnp.mean(values * values, axis=-1, keepdims=True) + norm_eps)
            hid[rows, :] = (values * inverse * gain[...]).astype(bf16)
            stats[rows, :] = jnp.broadcast_to(inverse, (BLOCK, 128))
            return carry

        lax.fori_loop(0, SECTIONS, norm, 0)
        for j in (4, 5, 1, 3, 7, 2, 6):
            for copy in hidden_send(j):
                copy.start()
        hmine[...] = hid[(SECTIONS - 1) * BLOCK :, :]
        smine[...] = stats[(SECTIONS - 1) * BLOCK :, :]

    def sender_slice(j):
        ky, kx = j // 2, j % 2
        return y_peer(y, ky) * 2 + flip(xh, kx)

    forwards = []
    for j in (2, 6, 1, 4, 3, 7, 5):
        part = hd.at[sender_slice(j), half]
        remote(part, part, hs.at[j], hrv.at[j], section_peer(j, True)).wait_recv()
        copy = remote(part, part, fs.at[j], fr.at[j], partner)
        copy.start()
        forwards.append(copy)
    mix_xl.wait_recv()
    mix_core[1].start()

    @pl.when(jnp.logical_not(root))
    def _():
        for copy in hidden_send(1):
            copy.wait_recv()

    def four(n):
        return dev(y, xh, z, flip(xl, n // 2), flip(c, n % 2))

    hid_sends = []
    for n in range(4):
        peer_column = flip(xl, n // 2) * 2 + flip(c, n % 2)
        src = hmine.at[:, pl.ds(pl.multiple_of(peer_column * 512, 512), 512)]
        if n == 0:
            copy = pltpu.make_async_copy(src, ghid.at[0], nr.at[0])
        else:
            copy = remote(src, ghid.at[n], ns.at[n], nr.at[n], four(n))
        copy.start()
        hid_sends.append(copy)
    for copy in forwards:
        copy.wait_recv()

    def logits(n, carry):
        lg[:, pl.ds(pl.multiple_of(n * SLICE, SLICE), SLICE)] = dot(hmine[...], hd[n], NT)
        return carry

    lax.fori_loop(0, SECTIONS, logits, 0)
    values = lg[...]
    shifted = jnp.exp(values - jnp.max(values, axis=1, keepdims=True))
    predicted = shifted / jnp.sum(shifted, axis=1, keepdims=True)
    columns_ = lax.broadcasted_iota(jnp.int32, (BLOCK, VOCAB), 1)
    lcb[...] = jnp.where(targets[...] == columns_, predicted - 1.0, predicted).astype(bf16)

    mine = pl.ds(pl.multiple_of(section * BLOCK, BLOCK), BLOCK)
    log_sends = []
    for j in range(8):
        peer_section = sender_slice(j)
        src = lcb.at[:, pl.ds(pl.multiple_of(peer_section * SLICE, SLICE), SLICE)]
        dst = alog.at[0, mine]
        if j == 0:
            copy = pltpu.make_async_copy(src, dst, lr.at[0])
        else:
            copy = remote(src, dst, ls.at[j], lr.at[j], section_peer(j))
        copy.start()
        log_sends.append(copy)

    def back(n, carry):
        cols = pl.ds(pl.multiple_of(n * 256, 256), 256)
        total = jnp.zeros((BLOCK, 256), f32)
        for s in range(SECTIONS):
            total += jnp.dot(
                lcb[:, s * SLICE : (s + 1) * SLICE], hd[s, :, cols], preferred_element_type=f32
            )
        hc[:, cols] = total
        return carry

    lax.fori_loop(0, WIDTH // 256, back, 0)
    scaled = hc[...] * gain[...]
    unit = hmine[...].astype(f32) / gain[...]
    inverse = smine[:, :1]
    along = jnp.mean(scaled * unit, axis=-1, keepdims=True)
    cotb[...] = (inverse * (scaled - unit * along)).astype(bf16)

    def offset(c_, part):
        low = (0, 1)[part]
        high = (-1, 2)[part]
        return sigma * (low + (high - low) * c_)

    def column_block(z_, xl_, c_, part):
        return ((z_ + offset(c_, part) + 8) % 8) * 2 + xl_

    cot_sends = []
    for m in (4, 5, 6, 7, 2, 3, 1, 0):
        z_, xl_, c_ = member(m)
        for part in range(2):
            block = column_block(z_, xl_, c_, part)
            src = cotb.at[:, pl.ds(pl.multiple_of(block * 128, 128), 128)]
            dst = gcot.at[m, :, pl.ds(part * 128, 128)]
            if m == 0:
                copy = pltpu.make_async_copy(src, dst, gr.at[m, part])
            else:
                copy = remote(src, dst, gs.at[m, part], gr.at[m, part], dev(y, xh, z_, xl_, c_))
            copy.start()
            cot_sends.append((m, copy))

    mix_z.wait_recv()
    mix_diag.start()
    mix_core[2].start()

    for m, copy in cot_sends:
        if m == 0:
            copy.wait()
        else:
            copy.wait_recv()
    all_sends = []
    for j in (6, 7, 4, 5, 1, 2, 3, 0):
        dst = bcot.at[:, mine]
        if j == 0:
            copy = pltpu.make_async_copy(gcot, dst, cr.at[0])
        else:
            copy = remote(gcot, dst, cs.at[j], cr.at[j], section_peer(j))
        copy.start()
        all_sends.append((j, copy))

    for j, copy in enumerate(log_sends):
        if j == 0:
            copy.wait()
        else:
            copy.wait_recv()
    log_group = []
    for n in range(1, 4):
        copy = remote(alog.at[0], alog.at[n], vs.at[n], vr.at[n], four(n))
        copy.start()
        log_group.append(copy)
    for n, copy in enumerate(hid_sends):
        if n == 0:
            copy.wait()
        else:
            copy.wait_recv()
    hid_all = []
    for j in (6, 7, 4, 5, 1, 2, 3, 0):
        dst = bhid.at[:, mine]
        if j == 0:
            copy = pltpu.make_async_copy(ghid, dst, wr.at[0])
        else:
            copy = remote(ghid, dst, ws.at[j], wr.at[j], section_peer(j))
        copy.start()
        hid_all.append((j, copy))

    mix_diag.wait_recv()
    mix_core[3].start()
    for copy in mix_core:
        copy.wait_recv()
    own_ids.wait()
    for copy in ids_sends:
        copy.wait_recv()
    for j, copy in all_sends:
        if j == 0:
            copy.wait()
        else:
            copy.wait_recv()

    def product(n, carry):
        cols = pl.ds(pl.multiple_of(n * 256, 256), 256)
        total = jnp.zeros((256, 256), f32)
        for m in range(8):
            total += dot(bcot[m], mix[m, :, cols], TN)
        psum[:, cols] = total
        psend[:, cols] = total.astype(bf16)
        return carry

    lax.fori_loop(0, WIDTH // 256, product, 0)

    def owner(part, c_):
        return dev(y, xh, (z + offset(c, part) + 8) % 8, xl, c_)

    def partial_rows(part, c_):
        return pl.ds((part * 2 + c_) * OWNED, OWNED)

    def far_copy(part, slot, c_):
        return remote(
            psend.at[partial_rows(part, c_)], rs.at[slot], rss.at[part, c_], rsr.at[slot], owner(part, c_)
        )

    near_copy = remote(psum.at[partial_rows(0, 1)], rs0, rss.at[0, 1], rsr.at[3], partner)

    @pl.when(c == 0)
    def _():
        far_copy(1, 1, 0).start()
        far_copy(1, 1, 1).start()
        near_copy.start()
        rs0[...] = psum[:OWNED, :]

    @pl.when(c == 1)
    def _():
        far_copy(1, 2, 0).start()
        far_copy(1, 2, 1).start()
        far_copy(0, 0, 0).start()
        far_copy(0, 0, 1).start()

    rows_ = section * SLICE + lax.broadcasted_iota(jnp.int32, (SLICE, TOKENS), 0)
    embed = jnp.zeros((SLICE, 256), f32)
    for m in range(8):
        marks = (idsb[m, :1, :] == rows_).astype(f32).astype(bf16)
        embed += jnp.dot(marks, bcot[m], preferred_element_type=f32)
    tile_e[...] = embed.reshape(REPLICAS, 8, 256)

    blocks = [column_block(z, xl, c, part) for part in range(2)]

    def embed_copy(target, part):
        cols = pl.ds(pl.multiple_of(blocks[part] * 128, 128), 128)
        return tile_e.at[target, :, pl.ds(part * 128, 128)], er.at[z % 4, :, cols]

    def send_embed(k, carry):
        target = (replica + k) % REPLICAS
        for part in range(2):
            src, dst = embed_copy(target, part)
            remote(src, dst, es.at[0], erv.at[0], (section, target)).start()
        return carry

    lax.fori_loop(1, REPLICAS, send_embed, 0)
    for part in range(2):
        src, dst = embed_copy(replica, part)
        pltpu.make_async_copy(src, dst, erv.at[0]).start()

    for copy in log_group:
        copy.wait_recv()
    for j, copy in hid_all:
        if j == 0:
            copy.wait()
        else:
            copy.wait_recv()

    head = jnp.zeros((SLICE, 512), f32)
    for n in range(4):
        head += dot(alog[n], bhid[n], TN)
    tile_h[...] = head.reshape(REPLICAS, 8, 512)
    head_cols = pl.ds(pl.multiple_of((xl * 2 + c) * 512, 512), 512)

    def send_head(k, carry):
        target = (replica + k) % REPLICAS
        remote(tile_h.at[target], hr.at[z, :, head_cols], zs.at[0], zr.at[0], (section, target)).start()
        return carry

    lax.fori_loop(1, REPLICAS, send_head, 0)
    pltpu.make_async_copy(tile_h.at[replica], hr.at[z, :, head_cols], zr.at[0]).start()

    @pl.when(c == 1)
    def _():
        near_copy.wait_recv()

    for slot in range(3):
        far_copy(1, slot, 0).wait_recv()
    out_grad[...] = (
        rs0[...] + rs[0].astype(f32) + rs[1].astype(f32) + rs[2].astype(f32)
    )
    pltpu.make_async_copy(er, er, erv.at[0]).wait()
    embed_grad[...] = er[0] + er[1] + er[2] + er[3]
    pltpu.make_async_copy(hr, hr, zr.at[0]).wait()
    total = hr[0]
    for k in range(1, 8):
        total += hr[k]
    head_grad[...] = total

    for copy in head_sends + forwards + mix_core + ids_sends + log_group + [mix_xl, mix_z, mix_diag]:
        copy.wait_send()
    for copies in (hid_sends, log_sends):
        for copy in copies[1:]:
            copy.wait_send()
    for copies in (cot_sends, all_sends, hid_all):
        for index, copy in copies:
            if index:
                copy.wait_send()

    @pl.when(root)
    def _():
        for j in range(1, 8):
            for copy in hidden_send(j):
                copy.wait_send()

    @pl.when(c == 0)
    def _():
        far_copy(1, 1, 0).wait_send()
        far_copy(1, 1, 1).wait_send()
        near_copy.wait_send()

    @pl.when(c == 1)
    def _():
        for part in range(2):
            for c_ in range(2):
                far_copy(part, 0, c_).wait_send()

    sent = tile_e.at[pl.ds(0, REPLICAS - 1)]
    pltpu.make_async_copy(sent, sent, es.at[0]).wait()
    sent = tile_h.at[pl.ds(0, REPLICAS - 1)]
    pltpu.make_async_copy(sent, sent, zs.at[0]).wait()


def gradients(wide, mixed, head, weight, gain, targets, ids):
    dma = pltpu.SemaphoreType.DMA
    vm = pltpu.VMEM
    any_ = pl.BlockSpec(memory_space=pl.ANY)
    vmem = pl.BlockSpec(memory_space=pltpu.VMEM)
    return pl.pallas_call(
        kernel,
        out_shape=(
            jax.ShapeDtypeStruct((OWNED, WIDTH), f32),
            jax.ShapeDtypeStruct((8, WIDTH), f32),
            jax.ShapeDtypeStruct((8, WIDTH), f32),
        ),
        in_specs=[any_] * 4 + [vmem] * 3,
        out_specs=(vmem,) * 3,
        scratch_shapes=[
            vm((8, TOKENS, WIDTH), bf16),
            vm((SECTIONS, SLICE, WIDTH), bf16),
            vm((8, 256, WIDTH), bf16),
            vm((TOKENS, WIDTH), bf16),
            vm((TOKENS, WIDTH), f32),
            vm((TOKENS, WIDTH), bf16),
            vm((TOKENS, 128), f32),
            vm((BLOCK, WIDTH), bf16),
            vm((BLOCK, 128), f32),
            vm((BLOCK, VOCAB), f32),
            vm((BLOCK, VOCAB), bf16),
            vm((BLOCK, WIDTH), f32),
            vm((BLOCK, WIDTH), bf16),
            vm((8, BLOCK, 256), bf16),
            vm((8, TOKENS, 256), bf16),
            vm((4, BLOCK, 512), bf16),
            vm((4, TOKENS, 512), bf16),
            vm((4, TOKENS, SLICE), bf16),
            vm((8, 8, TOKENS), jnp.int32),
            vm((256, WIDTH), f32),
            vm((256, WIDTH), bf16),
            vm((3, OWNED, WIDTH), bf16),
            vm((OWNED, WIDTH), f32),
            vm((REPLICAS, 8, 256), f32),
            vm((REPLICAS, 8, 512), f32),
            vm((4, 8, WIDTH), f32),
            vm((8, 8, WIDTH), f32),
            dma((12,)),
            dma((8,)), dma((8,)),
            dma((8,)), dma((8,)),
            dma((8,)), dma((8,)),
            dma((4,)), dma((4,)),
            dma((2, 8)), dma((2,)),
            dma((8,)), dma((8,)),
            dma((8, 2)), dma((8, 2)),
            dma((8,)), dma((8,)),
            dma((8,)), dma((8,)),
            dma((4,)), dma((4,)),
            dma((8,)), dma((8,)),
            dma((2, 2)), dma((4,)),
            dma((1,)), dma((1,)),
            dma((1,)), dma((1,)),
        ],
        compiler_params=pltpu.CompilerParams(
            collective_id=0, has_side_effects=True, vmem_limit_bytes=60 * 2**20
        ),
    )(wide, mixed, head, weight, gain, targets, ids)


def adam_update(master, first, second, gradient):
    first_next = beta_first * first + (1.0 - beta_first) * gradient
    second_next = beta_second * second + (1.0 - beta_second) * gradient * gradient
    master_next = master - learning_rate * (
        first_next / (jnp.sqrt(second_next) + adam_eps) + decay_rate * master
    )
    return (master_next, first_next, second_next)


def per_device(
    block_inputs, mixed_inputs, token_ids, target_ids, final_gain, out_weight, head_weight,
    out_master, out_first, out_second, head_master, head_first, head_second,
    embed_master, embed_first, embed_second,
):
    section = lax.axis_index("section")
    targets = lax.dynamic_slice_in_dim(target_ids.reshape(TOKENS, 1), section * BLOCK, BLOCK, 0)
    ids = jnp.broadcast_to(token_ids.reshape(1, TOKENS), (8, TOKENS))
    out_gradient, head_gradient, embed_gradient = gradients(
        block_inputs.reshape(TOKENS, WIDTH),
        mixed_inputs.reshape(TOKENS, WIDTH),
        head_weight,
        out_weight.reshape(WIDTH, WIDTH),
        final_gain.reshape(1, WIDTH),
        targets,
        ids,
    )
    return (
        *adam_update(out_master, out_first, out_second, out_gradient.reshape(out_master.shape)),
        *adam_update(head_master, head_first, head_second, head_gradient),
        *adam_update(embed_master, embed_first, embed_second, embed_gradient),
    )


def solution(mesh):
    tokens = P("section", None, "dp", None)
    rows = P("section", "dp", None)
    vocabulary = P(("section", "dp"), None)
    in_specs = (
        tokens, tokens, P(None, "dp"), P(None, "dp"), P(), P("section", None, None), P("section", None),
        rows, rows, rows, *(vocabulary,) * 6,
    )
    out_specs = (rows, rows, rows, *(vocabulary,) * 6)
    return jax.shard_map(
        per_device, mesh=mesh, in_specs=in_specs, out_specs=out_specs, check_vma=False
    )
```

```python
import jax
import jax.numpy as jnp
from jax import lax
from jax.experimental import pallas as pl
from jax.experimental.pallas import tpu as pltpu
from jax.sharding import PartitionSpec as P

norm_eps = 1e-05
beta_first = 0.9
beta_second = 0.95
adam_eps = 1e-05
learning_rate = 0.0003
decay_rate = 0.1
MESH = pl.DeviceIdType.MESH
bf16, f32 = jnp.bfloat16, jnp.float32
SECTIONS, REPLICAS = 8, 32
TOKENS, WIDTH, VOCAB = 256, 2048, 2048
BLOCK = TOKENS // SECTIONS
SLICE = VOCAB // SECTIONS
OWNED = 64
NT = (((1,), (1,)), ((), ()))
TN = (((0,), (0,)), ((), ()))


def dot(a, b, dims):
    return lax.dot_general(a, b, dims, preferred_element_type=f32)


def y_peer(y, k):
    return (y, y + 1 - 2 * (y % 2), (y + 2) % 4, 3 - y)[k]


def flip(value, k):
    return 1 - value if k else value


def kernel(
    wide_hbm, mixed_hbm, head_hbm, weight_hbm, gain_in, target_ids, token_ids,
    out_grad, head_grad, embed_grad,
    mix, hd, wbuf, wide, final, hid, stats, hmine, smine, lg, lcb, hc, cotb,
    gcot, bcot, ghid, bhid, alog, idsb, gain, psum, psend, rs, rs0, tile_e, tile_h, er, hr,
    loc, hs, hrv, fs, fr, ms, mr, ns, nr, ts, tr, ls, lr, gs, gr, cs, cr, is_, ir,
    vs, vr, ws, wr, rss, rsr, es, erv, zs, zr, fms, fmr,
):
    section = lax.axis_index("section")
    replica = lax.axis_index("dp")
    y, xh = section // 2, section % 2
    z, xl, c = replica // 4, (replica // 2) % 2, replica % 2
    sigma = 1 - 2 * (z % 2)
    root = section == SECTIONS - 1

    def dev(y_, xh_, z_, xl_, c_):
        return (y_ * 2 + xh_, z_ * 4 + xl_ * 2 + c_)

    def section_peer(j, cross=False):
        ky, kx = j // 2, j % 2
        return dev(y_peer(y, ky), flip(xh, kx), z, flip(xl, kx) if cross else xl, c)

    def member(m):
        kz, kl, kc = m // 4, (m // 2) % 2, m % 2
        return (z + 4 * kz) % 8, flip(xl, kl), flip(c, kc)

    def remote(src, dst, send, recv, device):
        return pltpu.make_async_remote_copy(
            src_ref=src, dst_ref=dst, send_sem=send, recv_sem=recv,
            device_id=device, device_id_type=MESH,
        )

    load_mix = pltpu.make_async_copy(mixed_hbm, mix.at[0], loc.at[0])
    load_head = pltpu.make_async_copy(head_hbm, hd.at[section], loc.at[1])
    load_mix.start()
    load_head.start()
    load_wide = pltpu.make_async_copy(wide_hbm, wide, loc.at[2])

    def load_weight(n):
        return pltpu.make_async_copy(weight_hbm.at[pl.ds(n * 256, 256)], wbuf.at[n], loc.at[4 + n])

    @pl.when(root)
    def _():
        load_wide.start()
        for n in range(8):
            load_weight(n).start()

    barrier = pltpu.get_barrier_semaphore()
    for j in range(1, 8):
        pl.semaphore_signal(barrier, inc=1, device_id=section_peer(j), device_id_type=MESH)
        if j % 2:
            pl.semaphore_signal(barrier, inc=1, device_id=section_peer(j, True), device_id_type=MESH)

    def greet(k, carry):
        pl.semaphore_signal(
            barrier, inc=1, device_id=(section, (replica + k) % REPLICAS), device_id_type=MESH
        )
        return carry

    lax.fori_loop(1, REPLICAS, greet, 0)
    pl.semaphore_wait(barrier, 7 + 4 + REPLICAS - 1)

    half = pl.ds(pl.multiple_of(c * 128, 128), 128)
    def sender_slice(j):
        return y_peer(y, j // 2) * 2 + flip(xh, j % 2)

    head_sends = {}

    def head_send(slot, source, peer):
        part = hd.at[sender_slice(source), half]
        copy = remote(part, part, hs.at[slot], hrv.at[slot], section_peer(peer, True))
        copy.start()
        head_sends[slot] = copy

    load_head.wait()
    for j in (1, 2, 6):
        head_send(j, 0, j)
    load_mix.wait()
    partner = dev(y, xh, z, xl, 1 - c)

    def mix_copy(src, dst, device):
        return remote(mix.at[src], mix.at[dst], ms.at[dst], mr.at[dst], device)

    mix_xl = mix_copy(0, 2, dev(y, xh, z, 1 - xl, c))
    mix_core = [mix_copy(m, m + 1, partner) for m in (0, 2)]

    def far_mix(src, dst, device):
        rows = [pl.ds(k * 64, 64) for k in range(4)]
        return [
            remote(mix.at[src, r], mix.at[dst, r], fms.at[dst - 4, k], fmr.at[dst - 4, k], device)
            for k, r in enumerate(rows)
        ]

    mix_z = far_mix(0, 4, dev(y, xh, (z + 4) % 8, xl, c))
    mix_diag = far_mix(4, 6, dev(y, xh, z, 1 - xl, c))
    core_z = far_mix(4, 5, partner)
    core_diag = far_mix(6, 7, partner)
    for copy in mix_z:
        copy.start()
    mix_core[0].start()
    idsb[0] = jnp.broadcast_to(
        jnp.concatenate([token_ids[b : b + 1, :] for b in range(4)], axis=1), (8, TOKENS)
    )
    gain[...] = gain_in[...].reshape(1, WIDTH)
    ids_sends = []
    for m in range(1, 8):
        copy = remote(idsb.at[0], idsb.at[m], is_.at[m], ir.at[m], dev(y, xh, *member(m)))
        copy.start()
        ids_sends.append(copy)

    def hidden_send(j):
        ky, kx = j // 2, j % 2
        peer = section_peer(j)
        rows = pl.ds(pl.multiple_of(peer[0] * BLOCK, BLOCK), BLOCK)
        return (
            remote(hid.at[rows], hmine, ts.at[0, j], tr.at[0], peer),
            remote(stats.at[rows], smine, ts.at[1, j], tr.at[1], peer),
        )

    @pl.when(root)
    def _():
        load_wide.wait()
        for n in range(8):
            load_weight(n).wait()

        def columns(n, carry):
            cols = pl.ds(pl.multiple_of(n * 256, 256), 256)
            final[:, cols] = dot(mix[0], wbuf[n], NT) + wide[:, cols].astype(f32)
            return carry

        lax.fori_loop(0, 8, columns, 0)

        def norm(b, carry):
            rows = pl.ds(pl.multiple_of(b * BLOCK, BLOCK), BLOCK)
            values = final[rows, :]
            inverse = lax.rsqrt(jnp.mean(values * values, axis=-1, keepdims=True) + norm_eps)
            hid[rows, :] = (values * inverse * gain[...]).astype(bf16)
            stats[rows, :] = jnp.broadcast_to(inverse, (BLOCK, 128))
            return carry

        lax.fori_loop(0, SECTIONS, norm, 0)
        for j in (4, 5, 1, 3, 7, 2, 6):
            for copy in hidden_send(j):
                copy.start()
        hmine[...] = hid[(SECTIONS - 1) * BLOCK :, :]
        smine[...] = stats[(SECTIONS - 1) * BLOCK :, :]

    head_send(4, 0, 4)
    mix_xl.start()

    forwards = {}

    def pass_on(j):
        part = hd.at[sender_slice(j), half]
        remote(part, part, hs.at[j], hrv.at[j], section_peer(j, True)).wait_recv()
        copy = remote(part, part, fs.at[j], fr.at[j], partner)
        copy.start()
        forwards[j] = copy

    def pass_far(k):
        mix_z[k].wait_recv()
        mix_diag[k].start()
        core_z[k].start()

    pass_on(1)
    head_send(3, 1, 2)
    head_send(7, 1, 6)
    pass_on(2)
    pass_on(6)
    pass_far(0)
    pass_on(4)
    head_send(5, 4, 1)
    pass_far(1)

    @pl.when(jnp.logical_not(root))
    def _():
        for copy in hidden_send(1):
            copy.wait_recv()

    hid_sends = []
    for m in range(8):
        z_, xl_, c_ = member(m)
        block = (z_ // 4) * 4 + xl_ * 2 + c_
        src = hmine.at[:, pl.ds(pl.multiple_of(block * 256, 256), 256)]
        if m == 0:
            copy = pltpu.make_async_copy(src, ghid.at[0], nr.at[0])
        else:
            copy = remote(src, ghid.at[m], ns.at[m], nr.at[m], dev(y, xh, z_, xl_, c_))
        copy.start()
        hid_sends.append(copy)

    def logits(j):
        n = sender_slice(j)
        lg[:, pl.ds(pl.multiple_of(n * SLICE, SLICE), SLICE)] = dot(hmine[...], hd[n], NT)

    logits(0)
    for j in (1, 2, 6, 4):
        forwards[j].wait_recv()
        logits(j)
    for j in (3, 7, 5):
        pass_on(j)
    for j in (3, 7, 5):
        forwards[j].wait_recv()
        logits(j)
    values = lg[...]
    shifted = jnp.exp(values - jnp.max(values, axis=1, keepdims=True))
    predicted = shifted / jnp.sum(shifted, axis=1, keepdims=True)
    columns_ = lax.broadcasted_iota(jnp.int32, (BLOCK, VOCAB), 1)
    batch_row = target_ids[pl.ds(section // 2, 1), :].astype(f32)
    lanes = lax.broadcasted_iota(jnp.int32, (BLOCK, 64), 1)
    places = lax.broadcasted_iota(jnp.int32, (BLOCK, 64), 0) + (section % 2) * BLOCK
    targets = jnp.sum(
        jnp.where(lanes == places, jnp.broadcast_to(batch_row, (BLOCK, 64)), 0.0), axis=1, keepdims=True
    )
    lcb[...] = jnp.where(targets == columns_.astype(f32), predicted - 1.0, predicted).astype(bf16)

    mine = pl.ds(pl.multiple_of(section * BLOCK, BLOCK), BLOCK)
    log_sends = []
    for j in range(8):
        peer_section = sender_slice(j)
        src = lcb.at[:, pl.ds(pl.multiple_of(peer_section * SLICE, SLICE), SLICE)]
        dst = alog.at[0, mine]
        if j == 0:
            copy = pltpu.make_async_copy(src, dst, lr.at[0])
        else:
            copy = remote(src, dst, ls.at[j], lr.at[j], section_peer(j))
        copy.start()
        log_sends.append(copy)

    pass_far(2)

    def back(n, carry):
        cols = pl.ds(pl.multiple_of(n * 256, 256), 256)
        total = jnp.zeros((BLOCK, 256), f32)
        for s in range(SECTIONS):
            total += jnp.dot(
                lcb[:, s * SLICE : (s + 1) * SLICE], hd[s, :, cols], preferred_element_type=f32
            )
        hc[:, cols] = total
        return carry

    lax.fori_loop(0, WIDTH // 256, back, 0)
    scaled = hc[...] * gain[...]
    unit = hmine[...].astype(f32) / gain[...]
    inverse = smine[:, :1]
    along = jnp.mean(scaled * unit, axis=-1, keepdims=True)
    cotb[...] = (inverse * (scaled - unit * along)).astype(bf16)

    def offset(c_, part):
        low = (0, 1)[part]
        high = (-1, 2)[part]
        return sigma * (low + (high - low) * c_)

    def column_block(z_, xl_, c_, part):
        return ((z_ + offset(c_, part) + 8) % 8) * 2 + xl_

    cot_sends = []
    for m in (4, 5, 6, 7, 2, 3, 1, 0):
        z_, xl_, c_ = member(m)
        for part in range(2):
            block = column_block(z_, xl_, c_, part)
            src = cotb.at[:, pl.ds(pl.multiple_of(block * 128, 128), 128)]
            dst = gcot.at[m, :, pl.ds(part * 128, 128)]
            if m == 0:
                copy = pltpu.make_async_copy(src, dst, gr.at[m, part])
            else:
                copy = remote(src, dst, gs.at[m, part], gr.at[m, part], dev(y, xh, z_, xl_, c_))
            copy.start()
            cot_sends.append((m, copy))

    pass_far(3)
    mix_xl.wait_recv()
    mix_core[1].start()

    for n, copy in enumerate(hid_sends):
        if n == 0:
            copy.wait()
        else:
            copy.wait_recv()
    hid_all = []

    def gather_hidden(j):
        dst = bhid.at[:, mine]
        if j == 0:
            copy = pltpu.make_async_copy(ghid, dst, wr.at[0])
        else:
            copy = remote(ghid, dst, ws.at[j], wr.at[j], section_peer(j))
        copy.start()
        hid_all.append((j, copy))

    for j in (2, 6, 4, 0):
        gather_hidden(j)

    for m, copy in cot_sends:
        if m == 0:
            copy.wait()
        else:
            copy.wait_recv()
    all_sends = []
    for j in (6, 7, 4, 5, 1, 2, 3, 0):
        dst = bcot.at[:, mine]
        if j == 0:
            copy = pltpu.make_async_copy(gcot, dst, cr.at[0])
        else:
            copy = remote(gcot, dst, cs.at[j], cr.at[j], section_peer(j))
        copy.start()
        all_sends.append((j, copy))

    for j, copy in enumerate(log_sends):
        if j == 0:
            copy.wait()
        else:
            copy.wait_recv()
    def log_copy(src, dst, device):
        return remote(alog.at[src], alog.at[dst], vs.at[dst], vr.at[dst], device)

    log_far = [log_copy(0, m, dev(y, xh, *member(m))) for m in (4, 6, 2)]
    log_core = [log_copy(m, m + 1, partner) for m in (0, 2, 4, 6)]
    for copy in log_far + log_core[:1]:
        copy.start()
    for j in (3, 7, 5, 1):
        gather_hidden(j)

    for k in range(4):
        mix_diag[k].wait_recv()
        core_diag[k].start()
    for copy in mix_core + core_z + core_diag:
        copy.wait_recv()
    for copy in log_far:
        copy.wait_recv()
    for copy in log_core[1:]:
        copy.start()
    for copy in ids_sends:
        copy.wait_recv()
    for j, copy in all_sends:
        if j == 0:
            copy.wait()
        else:
            copy.wait_recv()

    rows_ = section * SLICE + lax.broadcasted_iota(jnp.int32, (SLICE, TOKENS), 0)
    embed = jnp.zeros((SLICE, 256), f32)
    for m in range(8):
        marks = (idsb[m, :1, :] == rows_).astype(f32).astype(bf16)
        embed += jnp.dot(marks, bcot[m], preferred_element_type=f32)
    tile_e[...] = embed.reshape(REPLICAS, 8, 256)

    blocks = [column_block(z, xl, c, part) for part in range(2)]

    def embed_copy(target, part):
        cols = pl.ds(pl.multiple_of(blocks[part] * 128, 128), 128)
        return tile_e.at[target, :, pl.ds(part * 128, 128)], er.at[z % 4, :, cols]

    def send_embed(k, carry):
        target = (replica + k) % REPLICAS
        for part in range(2):
            src, dst = embed_copy(target, part)
            remote(src, dst, es.at[0], erv.at[0], (section, target)).start()
        return carry

    lax.fori_loop(1, REPLICAS, send_embed, 0)
    for part in range(2):
        src, dst = embed_copy(replica, part)
        pltpu.make_async_copy(src, dst, erv.at[0]).start()

    def product(n, carry):
        cols = pl.ds(pl.multiple_of(n * 256, 256), 256)
        total = jnp.zeros((256, 256), f32)
        for m in range(8):
            total += dot(bcot[m], mix[m, :, cols], TN)
        psum[:, cols] = total
        psend[:, cols] = total.astype(bf16)
        return carry

    def owner(part, c_):
        return dev(y, xh, (z + offset(c, part) + 8) % 8, xl, c_)

    def partial_rows(part, c_):
        return pl.ds((part * 2 + c_) * OWNED, OWNED)

    def far_copy(part, slot, c_, h):
        cols = pl.ds(h * (WIDTH // 2), WIDTH // 2)
        return remote(
            psend.at[partial_rows(part, c_), cols], rs.at[slot, :, cols],
            rss.at[h, part, c_], rsr.at[h, slot], owner(part, c_),
        )

    def near_copy(h):
        cols = pl.ds(h * (WIDTH // 2), WIDTH // 2)
        return remote(
            psum.at[partial_rows(0, 1), cols], rs0.at[:, cols], rss.at[h, 0, 1], rsr.at[h, 3], partner
        )

    for h in range(2):
        lax.fori_loop(h * 4, h * 4 + 4, product, 0)

        @pl.when(c == 0)
        def _(h=h):
            far_copy(1, 1, 0, h).start()
            far_copy(1, 1, 1, h).start()
            near_copy(h).start()

        @pl.when(c == 1)
        def _(h=h):
            far_copy(1, 2, 0, h).start()
            far_copy(1, 2, 1, h).start()
            far_copy(0, 0, 0, h).start()
            far_copy(0, 0, 1, h).start()

    @pl.when(c == 0)
    def _():
        rs0[...] = psum[:OWNED, :]

    for copy in log_core:
        copy.wait_recv()
    for j, copy in hid_all:
        if j == 0:
            copy.wait()
        else:
            copy.wait_recv()

    head = jnp.zeros((SLICE, 256), f32)
    for m in range(8):
        head += dot(alog[m], bhid[m], TN)
    tile_h[...] = head.reshape(REPLICAS, 8, 256)
    head_block = (z // 4) * 4 + xl * 2 + c
    head_cols = pl.ds(pl.multiple_of(head_block * 256, 256), 256)

    def send_head(k, carry):
        target = (replica + k) % REPLICAS
        remote(
            tile_h.at[target], hr.at[z % 4, :, head_cols], zs.at[0], zr.at[0], (section, target)
        ).start()
        return carry

    lax.fori_loop(1, REPLICAS, send_head, 0)
    pltpu.make_async_copy(tile_h.at[replica], hr.at[z % 4, :, head_cols], zr.at[0]).start()

    @pl.when(c == 1)
    def _():
        for h in range(2):
            near_copy(h).wait_recv()

    for h in range(2):
        for slot in range(3):
            far_copy(1, slot, 0, h).wait_recv()
    out_grad[...] = (
        rs0[...] + rs[0].astype(f32) + rs[1].astype(f32) + rs[2].astype(f32)
    )
    pltpu.make_async_copy(er, er, erv.at[0]).wait()
    embed_grad[...] = er[0] + er[1] + er[2] + er[3]
    pltpu.make_async_copy(hr, hr, zr.at[0]).wait()
    head_grad[...] = hr[0] + hr[1] + hr[2] + hr[3]

    copies = [mix_xl, *head_sends.values(), *forwards.values()]
    copies += mix_core + mix_z + mix_diag + core_z + core_diag + ids_sends + log_far + log_core
    for copy in copies:
        copy.wait_send()
    for copies in (hid_sends, log_sends):
        for copy in copies[1:]:
            copy.wait_send()
    for copies in (cot_sends, all_sends, hid_all):
        for index, copy in copies:
            if index:
                copy.wait_send()

    @pl.when(root)
    def _():
        for j in range(1, 8):
            for copy in hidden_send(j):
                copy.wait_send()

    @pl.when(c == 0)
    def _():
        for h in range(2):
            far_copy(1, 1, 0, h).wait_send()
            far_copy(1, 1, 1, h).wait_send()
            near_copy(h).wait_send()

    @pl.when(c == 1)
    def _():
        for h in range(2):
            for part in range(2):
                for c_ in range(2):
                    far_copy(part, 0, c_, h).wait_send()

    sent = tile_e.at[pl.ds(0, REPLICAS - 1)]
    pltpu.make_async_copy(sent, sent, es.at[0]).wait()
    sent = tile_h.at[pl.ds(0, REPLICAS - 1)]
    pltpu.make_async_copy(sent, sent, zs.at[0]).wait()


def gradients(wide, mixed, head, weight, gain, target_ids, token_ids):
    dma = pltpu.SemaphoreType.DMA
    vm = pltpu.VMEM
    any_ = pl.BlockSpec(memory_space=pl.ANY)
    vmem = pl.BlockSpec(memory_space=pltpu.VMEM)
    return pl.pallas_call(
        kernel,
        out_shape=(
            jax.ShapeDtypeStruct((OWNED, WIDTH), f32),
            jax.ShapeDtypeStruct((8, WIDTH), f32),
            jax.ShapeDtypeStruct((8, WIDTH), f32),
        ),
        in_specs=[any_] * 4 + [vmem] * 3,
        out_specs=(vmem,) * 3,
        scratch_shapes=[
            vm((8, TOKENS, WIDTH), bf16),
            vm((SECTIONS, SLICE, WIDTH), bf16),
            vm((8, 256, WIDTH), bf16),
            vm((TOKENS, WIDTH), bf16),
            vm((TOKENS, WIDTH), f32),
            vm((TOKENS, WIDTH), bf16),
            vm((TOKENS, 128), f32),
            vm((BLOCK, WIDTH), bf16),
            vm((BLOCK, 128), f32),
            vm((BLOCK, VOCAB), f32),
            vm((BLOCK, VOCAB), bf16),
            vm((BLOCK, WIDTH), f32),
            vm((BLOCK, WIDTH), bf16),
            vm((8, BLOCK, 256), bf16),
            vm((8, TOKENS, 256), bf16),
            vm((8, BLOCK, 256), bf16),
            vm((8, TOKENS, 256), bf16),
            vm((8, TOKENS, SLICE), bf16),
            vm((8, 8, TOKENS), jnp.int32),
            vm((1, WIDTH), f32),
            vm((256, WIDTH), f32),
            vm((256, WIDTH), bf16),
            vm((3, OWNED, WIDTH), bf16),
            vm((OWNED, WIDTH), f32),
            vm((REPLICAS, 8, 256), f32),
            vm((REPLICAS, 8, 256), f32),
            vm((4, 8, WIDTH), f32),
            vm((4, 8, WIDTH), f32),
            dma((12,)),
            dma((8,)), dma((8,)),
            dma((8,)), dma((8,)),
            dma((8,)), dma((8,)),
            dma((8,)), dma((8,)),
            dma((2, 8)), dma((2,)),
            dma((8,)), dma((8,)),
            dma((8, 2)), dma((8, 2)),
            dma((8,)), dma((8,)),
            dma((8,)), dma((8,)),
            dma((8,)), dma((8,)),
            dma((8,)), dma((8,)),
            dma((2, 2, 2)), dma((2, 4)),
            dma((1,)), dma((1,)),
            dma((1,)), dma((1,)),
            dma((4, 4)), dma((4, 4)),
        ],
        compiler_params=pltpu.CompilerParams(
            collective_id=0, has_side_effects=True, vmem_limit_bytes=60 * 2**20
        ),
    )(wide, mixed, head, weight, gain, target_ids, token_ids)


def adam_update(master, first, second, gradient):
    first_next = beta_first * first + (1.0 - beta_first) * gradient
    second_next = beta_second * second + (1.0 - beta_second) * gradient * gradient
    master_next = master - learning_rate * (
        first_next / (jnp.sqrt(second_next) + adam_eps) + decay_rate * master
    )
    return (master_next, first_next, second_next)


def per_device(
    block_inputs, mixed_inputs, token_ids, target_ids, final_gain, out_weight, head_weight,
    out_master, out_first, out_second, head_master, head_first, head_second,
    embed_master, embed_first, embed_second,
):
    out_gradient, head_gradient, embed_gradient = gradients(
        block_inputs.reshape(TOKENS, WIDTH),
        mixed_inputs.reshape(TOKENS, WIDTH),
        head_weight,
        out_weight.reshape(WIDTH, WIDTH),
        final_gain,
        target_ids,
        token_ids,
    )
    return (
        *adam_update(out_master, out_first, out_second, out_gradient.reshape(out_master.shape)),
        *adam_update(head_master, head_first, head_second, head_gradient),
        *adam_update(embed_master, embed_first, embed_second, embed_gradient),
    )


def solution(mesh):
    tokens = P("section", None, "dp", None)
    rows = P("section", "dp", None)
    vocabulary = P(("section", "dp"), None)
    in_specs = (
        tokens, tokens, P(None, "dp"), P(None, "dp"), P(), P("section", None, None), P("section", None),
        rows, rows, rows, *(vocabulary,) * 6,
    )
    out_specs = (rows, rows, rows, *(vocabulary,) * 6)
    return jax.shard_map(
        per_device, mesh=mesh, in_specs=in_specs, out_specs=out_specs, check_vma=False
    )
```

```python
import jax
import jax.numpy as jnp
from jax import lax
from jax.experimental import pallas as pl
from jax.experimental.pallas import tpu as pltpu
from jax.sharding import PartitionSpec as P

norm_eps = 1e-05
beta_first = 0.9
beta_second = 0.95
adam_eps = 1e-05
learning_rate = 0.0003
decay_rate = 0.1
MESH = pl.DeviceIdType.MESH
bf16, f32 = jnp.bfloat16, jnp.float32
SECTIONS, REPLICAS = 8, 32
TOKENS, WIDTH, VOCAB = 256, 2048, 2048
BLOCK = TOKENS // SECTIONS
SLICE = VOCAB // SECTIONS
OWNED = 64
NT = (((1,), (1,)), ((), ()))
TN = (((0,), (0,)), ((), ()))


def dot(a, b, dims):
    return lax.dot_general(a, b, dims, preferred_element_type=f32)


def y_peer(y, k):
    return (y, y + 1 - 2 * (y % 2), (y + 2) % 4, 3 - y)[k]


def flip(value, k):
    return 1 - value if k else value


def kernel(
    wide_hbm, mixed_hbm, head_hbm, weight_hbm, gain_in, target_ids, token_ids,
    out_grad, head_grad, embed_grad,
    mix, hd, wbuf, wide, final, hid, stats, hmine, smine, lg, lcb, hc, cotb,
    gcot, bcot, ghid, bhid, alog, idsb, gain, psum, psend, rs, rs0, tile_e, tile_h, er, hr,
    loc, hs, hrv, fs, fr, ms, mr, ns, nr, ts, tr, ls, lr, gs, gr, cs, cr, is_, ir,
    vs, vr, ws, wr, rss, rsr, es, erv, zs, zr, fms, fmr,
):
    section = lax.axis_index("section")
    replica = lax.axis_index("dp")
    y, xh = section // 2, section % 2
    z, xl, c = replica // 4, (replica // 2) % 2, replica % 2
    sigma = 1 - 2 * (z % 2)
    root = section == SECTIONS - 1

    def dev(y_, xh_, z_, xl_, c_):
        return (y_ * 2 + xh_, z_ * 4 + xl_ * 2 + c_)

    def section_peer(j, cross=False):
        ky, kx = j // 2, j % 2
        return dev(y_peer(y, ky), flip(xh, kx), z, flip(xl, kx) if cross else xl, c)

    def member(m):
        kz, kl, kc = m // 4, (m // 2) % 2, m % 2
        return (z + 4 * kz) % 8, flip(xl, kl), flip(c, kc)

    def head_member(m):
        near = (z + (m // 2) % 2 * (1 - 2 * (z % 2))) % 8
        return (near + 4 * (m // 4)) % 8, xl, flip(c, m % 2)

    def head_column(z_, c_):
        return (z_ // 4) * 4 + (z_ % 2) * 2 + c_

    def remote(src, dst, send, recv, device):
        return pltpu.make_async_remote_copy(
            src_ref=src, dst_ref=dst, send_sem=send, recv_sem=recv,
            device_id=device, device_id_type=MESH,
        )

    load_mix = pltpu.make_async_copy(mixed_hbm, mix.at[0], loc.at[0])
    load_head = pltpu.make_async_copy(head_hbm, hd.at[section], loc.at[1])
    load_mix.start()
    load_head.start()
    load_wide = pltpu.make_async_copy(wide_hbm, wide, loc.at[2])

    def load_weight(n):
        return pltpu.make_async_copy(weight_hbm.at[pl.ds(n * 256, 256)], wbuf.at[n], loc.at[4 + n])

    @pl.when(root)
    def _():
        load_wide.start()
        for n in range(8):
            load_weight(n).start()

    barrier = pltpu.get_barrier_semaphore()
    for j in range(1, 8):
        pl.semaphore_signal(barrier, inc=1, device_id=section_peer(j), device_id_type=MESH)
        if j % 2:
            pl.semaphore_signal(barrier, inc=1, device_id=section_peer(j, True), device_id_type=MESH)

    def greet(k, carry):
        pl.semaphore_signal(
            barrier, inc=1, device_id=(section, (replica + k) % REPLICAS), device_id_type=MESH
        )
        return carry

    lax.fori_loop(1, REPLICAS, greet, 0)
    pl.semaphore_wait(barrier, 7 + 4 + REPLICAS - 1)

    half = pl.ds(pl.multiple_of(c * 128, 128), 128)
    def sender_slice(j):
        return y_peer(y, j // 2) * 2 + flip(xh, j % 2)

    HALVES = ((0, 64), (64, 128))
    head_sends = {}

    def head_copy(slot, source, peer, rows=(0, 128)):
        first, last = rows
        part = hd.at[
            sender_slice(source), pl.ds(pl.multiple_of(c * 128 + first, 16), last - first)
        ]
        lane = int(first > 0)
        return remote(part, part, hs.at[lane, slot], hrv.at[lane, slot], section_peer(peer, True))

    def head_send(slot, source, peer, rows=(0, 128)):
        copy = head_copy(slot, source, peer, rows)
        copy.start()
        head_sends[slot, rows] = copy

    load_head.wait()
    for j in (1, 2, 6):
        head_send(j, 0, j)
    load_mix.wait()
    partner = dev(y, xh, z, xl, 1 - c)

    def mix_copy(src, dst, device):
        return remote(mix.at[src], mix.at[dst], ms.at[dst], mr.at[dst], device)

    mix_xl = [
        remote(
            mix.at[0, pl.ds(h * 128, 128)], mix.at[2, pl.ds(h * 128, 128)],
            fms.at[1 + h, 0], fmr.at[1 + h, 0], dev(y, xh, z, 1 - xl, c),
        )
        for h in range(2)
    ]
    mix_core = [mix_copy(m, m + 1, partner) for m in (0, 2)]

    def far_mix(src, dst, device):
        rows = [pl.ds(k * 64, 64) for k in range(4)]
        return [
            remote(mix.at[src, r], mix.at[dst, r], fms.at[dst, k], fmr.at[dst, k], device)
            for k, r in enumerate(rows)
        ]

    mix_z = far_mix(0, 4, dev(y, xh, (z + 4) % 8, xl, c))
    mix_diag = far_mix(4, 6, dev(y, xh, z, 1 - xl, c))
    core_z = far_mix(4, 5, partner)
    core_diag = far_mix(6, 7, partner)
    mix_z[0].start()
    mix_z[1].start()
    mix_xl[0].start()
    mix_core[0].start()
    idsb[0] = jnp.broadcast_to(
        jnp.concatenate([token_ids[b : b + 1, :] for b in range(4)], axis=1), (8, TOKENS)
    )
    gain[...] = gain_in[...].reshape(1, WIDTH)
    ids_sends = []
    for m in range(1, 8):
        copy = remote(idsb.at[0], idsb.at[m], is_.at[m], ir.at[m], dev(y, xh, *member(m)))
        copy.start()
        ids_sends.append(copy)

    def hidden_send(j):
        ky, kx = j // 2, j % 2
        peer = section_peer(j)
        rows = pl.ds(pl.multiple_of(peer[0] * BLOCK, BLOCK), BLOCK)
        return (
            remote(hid.at[rows], hmine, ts.at[0, j], tr.at[0], peer),
            remote(stats.at[rows], smine, ts.at[1, j], tr.at[1], peer),
        )

    @pl.when(root)
    def _():
        load_wide.wait()
        for n in range(8):
            load_weight(n).wait()

        def columns(n, carry):
            cols = pl.ds(pl.multiple_of(n * 256, 256), 256)
            final[:, cols] = dot(mix[0], wbuf[n], NT) + wide[:, cols].astype(f32)
            return carry

        lax.fori_loop(0, 8, columns, 0)

        def norm(b, carry):
            rows = pl.ds(pl.multiple_of(b * BLOCK, BLOCK), BLOCK)
            values = final[rows, :]
            inverse = lax.rsqrt(jnp.mean(values * values, axis=-1, keepdims=True) + norm_eps)
            hid[rows, :] = (values * inverse * gain[...]).astype(bf16)
            stats[rows, :] = jnp.broadcast_to(inverse, (BLOCK, 128))
            return carry

        lax.fori_loop(0, SECTIONS, norm, 0)
        for j in (4, 5, 1, 3, 7, 2, 6):
            for copy in hidden_send(j):
                copy.start()
        hmine[...] = hid[(SECTIONS - 1) * BLOCK :, :]
        smine[...] = stats[(SECTIONS - 1) * BLOCK :, :]

    for rows in HALVES:
        head_send(4, 0, 4, rows)
    mix_xl[1].start()

    forwards = {}

    SPLIT = ((0, 112), (112, 128))

    def pass_on(j):
        part = hd.at[sender_slice(j), half]
        for rows in {3: SPLIT, 7: SPLIT, 4: HALVES, 5: HALVES}.get(j, ((0, 128),)):
            head_copy(j, j, j, rows).wait_recv()
            if j == 4:
                head_send(5, 4, 1, rows)
        copy = remote(part, part, fs.at[j], fr.at[j], partner)
        copy.start()
        forwards[j] = copy

    def pass_far(k):
        mix_z[k].wait_recv()
        mix_diag[k].start()
        core_z[k].start()
        if k == 0:
            mix_z[2].start()

    pass_on(1)
    head_send(3, 1, 2, SPLIT[0])
    head_send(7, 1, 6, SPLIT[0])
    pass_on(2)
    head_send(3, 2, 1, SPLIT[1])
    pass_on(6)
    head_send(7, 6, 1, SPLIT[1])
    pass_far(0)
    pass_on(4)

    @pl.when(jnp.logical_not(root))
    def _():
        for copy in hidden_send(1):
            copy.wait_recv()

    mine = pl.ds(pl.multiple_of(section * BLOCK, BLOCK), BLOCK)
    hid_sends = []
    for m in range(8):
        z_, xl_, c_ = head_member(m)
        block = head_column(z_, c_)
        src = hmine.at[:, pl.ds(pl.multiple_of(block * 256, 256), 256)]
        if m == 0:
            copy = pltpu.make_async_copy(src, ghid.at[0], nr.at[0])
        else:
            copy = remote(src, ghid.at[m], ns.at[m], nr.at[m], dev(y, xh, z_, xl_, c_))
        copy.start()
        hid_sends.append(copy)
    mix_z[3].start()

    def logits(j):
        n = sender_slice(j)
        lg[:, pl.ds(pl.multiple_of(n * SLICE, SLICE), SLICE)] = dot(hmine[...], hd[n], NT)

    for j in (0, 1, 2, 6):
        if j:
            forwards[j].wait_recv()
        logits(j)
    pass_far(1)
    for j in (3, 7, 5):
        pass_on(j)
    for j in (4, 3, 7, 5):
        forwards[j].wait_recv()
        logits(j)
    values = lg[...]
    shifted = jnp.exp(values - jnp.max(values, axis=1, keepdims=True))
    predicted = shifted / jnp.sum(shifted, axis=1, keepdims=True)
    columns_ = lax.broadcasted_iota(jnp.int32, (BLOCK, VOCAB), 1)
    batch_row = target_ids[pl.ds(section // 2, 1), :].astype(f32)
    lanes = lax.broadcasted_iota(jnp.int32, (BLOCK, 64), 1)
    places = lax.broadcasted_iota(jnp.int32, (BLOCK, 64), 0) + (section % 2) * BLOCK
    targets = jnp.sum(
        jnp.where(lanes == places, jnp.broadcast_to(batch_row, (BLOCK, 64)), 0.0), axis=1, keepdims=True
    )
    lcb[...] = jnp.where(targets == columns_.astype(f32), predicted - 1.0, predicted).astype(bf16)

    log_sends = []
    for j in range(8):
        peer_section = sender_slice(j)
        src = lcb.at[:, pl.ds(pl.multiple_of(peer_section * SLICE, SLICE), SLICE)]
        dst = alog.at[0, mine]
        if j == 0:
            copy = pltpu.make_async_copy(src, dst, lr.at[0])
        else:
            copy = remote(src, dst, ls.at[j], lr.at[j], section_peer(j))
        copy.start()
        log_sends.append(copy)

    def block_rows(j):
        return pl.ds(pl.multiple_of(sender_slice(j) * BLOCK, BLOCK), BLOCK)

    for n, copy in enumerate(hid_sends):
        if n == 0:
            copy.wait()
        else:
            copy.wait_recv()

    hid_all = {}

    def gather_hidden(slot, src, rows, peer):
        dst = bhid.at[:, rows]
        if slot == 0:
            copy = pltpu.make_async_copy(src, dst, wr.at[0])
        else:
            copy = remote(src, dst, ws.at[slot], wr.at[slot], section_peer(peer))
        copy.start()
        hid_all[slot] = copy

    for j in (2, 6, 4, 0):
        gather_hidden(j, ghid, mine, j)
    def back(n, carry):
        cols = pl.ds(pl.multiple_of(n * 256, 256), 256)
        total = jnp.zeros((BLOCK, 256), f32)
        for s in range(SECTIONS):
            total += jnp.dot(
                lcb[:, s * SLICE : (s + 1) * SLICE], hd[s, :, cols], preferred_element_type=f32
            )
        hc[:, cols] = total
        return carry

    lax.fori_loop(0, WIDTH // 256, back, 0)
    scaled = hc[...] * gain[...]
    unit = hmine[...].astype(f32) / gain[...]
    inverse = smine[:, :1]
    along = jnp.mean(scaled * unit, axis=-1, keepdims=True)
    cotb[...] = (inverse * (scaled - unit * along)).astype(bf16)

    def offset(c_, part):
        low = (0, 1)[part]
        high = (-1, 2)[part]
        return sigma * (low + (high - low) * c_)

    def column_block(z_, xl_, c_, part):
        return ((z_ + offset(c_, part) + 8) % 8) * 2 + xl_

    cot_sends = []
    for m in (4, 5, 6, 7, 2, 3, 1, 0):
        z_, xl_, c_ = member(m)
        for part in range(2):
            block = column_block(z_, xl_, c_, part)
            src = cotb.at[:, pl.ds(pl.multiple_of(block * 128, 128), 128)]
            dst = gcot.at[m, :, pl.ds(part * 128, 128)]
            if m == 0:
                copy = pltpu.make_async_copy(src, dst, gr.at[m, part])
            else:
                copy = remote(src, dst, gs.at[m, part], gr.at[m, part], dev(y, xh, z_, xl_, c_))
            copy.start()
            cot_sends.append((m, copy))

    cot_all = {}

    def gather_cotangent(slot, part, src, rows, peer):
        members = pl.ds(part * 4, 4)
        dst = bcot.at[members, rows]
        if slot == 0:
            copy = pltpu.make_async_copy(src.at[members], dst, cr.at[part, 0])
        else:
            copy = remote(
                src.at[members, rows] if src is bcot else src.at[members],
                dst, cs.at[part, slot], cr.at[part, slot], section_peer(peer),
            )
        copy.start()
        cot_all[slot, part] = copy

    for part in range(2):
        for m, copy in cot_sends:
            if m // 4 == part:
                copy.wait() if m == 0 else copy.wait_recv()
        for j in (1, 2, 6, 4, 0):
            gather_cotangent(j, part, gcot, mine, j)

    pass_far(2)
    for part in range(2):
        cot_all[1, part].wait_recv()
        for j in (2, 6, 4):
            gather_cotangent(j + 1, part, bcot, block_rows(1), j)

    pass_far(3)
    hid_all[0].wait()
    for j in (2, 6, 4):
        hid_all[j].wait_recv()
    for j in (0, 2, 6, 4):
        gather_hidden(j + 1, bhid.at[:, block_rows(j)], block_rows(j), 1)
    for j, copy in enumerate(log_sends):
        if j == 0:
            copy.wait()
        else:
            copy.wait_recv()
    def log_copy(src, dst, device):
        return remote(alog.at[src], alog.at[dst], vs.at[dst], vr.at[dst], device)

    log_far = [log_copy(0, m, dev(y, xh, *head_member(m))) for m in (4, 6, 2)]
    log_core = [log_copy(m, m + 1, partner) for m in (0, 2, 4, 6)]
    for copy in log_far + log_core[:1]:
        copy.start()

    for h in range(2):
        mix_xl[h].wait_recv()
    mix_core[1].start()
    for k in range(4):
        mix_diag[k].wait_recv()
        core_diag[k].start()
    for copy in mix_core + core_z + core_diag:
        copy.wait_recv()
    for copy in ids_sends:
        copy.wait_recv()
    for part in range(2):
        cot_all[0, part].wait()
        for j in (2, 6, 4, 3, 7, 5):
            cot_all[j, part].wait_recv()

    rows_ = section * SLICE + lax.broadcasted_iota(jnp.int32, (SLICE, TOKENS), 0)
    embed = jnp.zeros((SLICE, 256), f32)
    for m in range(8):
        marks = (idsb[m, :1, :] == rows_).astype(f32).astype(bf16)
        embed += jnp.dot(marks, bcot[m], preferred_element_type=f32)
    tile_e[...] = embed.reshape(REPLICAS, 8, 256)

    blocks = [column_block(z, xl, c, part) for part in range(2)]

    def embed_copy(target, part):
        cols = pl.ds(pl.multiple_of(blocks[part] * 128, 128), 128)
        return tile_e.at[target, :, pl.ds(part * 128, 128)], er.at[z % 4, :, cols]

    def send_embed(k, carry):
        target = (replica + k) % REPLICAS
        for part in range(2):
            src, dst = embed_copy(target, part)
            remote(src, dst, es.at[0], erv.at[0], (section, target)).start()
        return carry

    lax.fori_loop(1, REPLICAS, send_embed, 0)
    for part in range(2):
        src, dst = embed_copy(replica, part)
        pltpu.make_async_copy(src, dst, erv.at[0]).start()

    def product(n, carry):
        cols = pl.ds(pl.multiple_of(n * 256, 256), 256)
        total = jnp.zeros((256, 256), f32)
        for m in range(8):
            total += dot(bcot[m], mix[m, :, cols], TN)
        psum[:, cols] = total
        psend[:, cols] = total.astype(bf16)
        return carry

    def owner(part, c_):
        return dev(y, xh, (z + offset(c, part) + 8) % 8, xl, c_)

    def partial_rows(part, c_):
        return pl.ds((part * 2 + c_) * OWNED, OWNED)

    def far_copy(part, slot, c_, h):
        cols = pl.ds(h * (WIDTH // 2), WIDTH // 2)
        return remote(
            psend.at[partial_rows(part, c_), cols], rs.at[slot, :, cols],
            rss.at[h, part, c_], rsr.at[h, slot], owner(part, c_),
        )

    def near_copy(h):
        cols = pl.ds(h * (WIDTH // 2), WIDTH // 2)
        return remote(
            psum.at[partial_rows(0, 1), cols], rs0.at[:, cols], rss.at[h, 0, 1], rsr.at[h, 3], partner
        )

    for h in range(2):
        lax.fori_loop(h * 4, h * 4 + 4, product, 0)

        @pl.when(c == 0)
        def _(h=h):
            far_copy(1, 1, 0, h).start()
            far_copy(1, 1, 1, h).start()
            near_copy(h).start()

        @pl.when(c == 1)
        def _(h=h):
            far_copy(1, 2, 0, h).start()
            far_copy(1, 2, 1, h).start()
            far_copy(0, 0, 0, h).start()
            far_copy(0, 0, 1, h).start()

    @pl.when(c == 0)
    def _():
        rs0[...] = psum[:OWNED, :]

    for copy in log_far:
        copy.wait_recv()
    for copy in log_core[1:]:
        copy.start()
    for copy in log_core:
        copy.wait_recv()
    for j in (1, 3, 7, 5):
        hid_all[j].wait_recv()

    head = jnp.zeros((SLICE, 256), f32)
    for m in range(8):
        head += dot(alog[m], bhid[m], TN)
    tile_h[...] = head.reshape(REPLICAS, 8, 256)
    head_cols = pl.ds(pl.multiple_of(head_column(z, c) * 256, 256), 256)
    head_class = xl * 2 + (z // 2) % 2

    def send_head(k, carry):
        target = (replica + k) % REPLICAS
        remote(
            tile_h.at[target], hr.at[head_class, :, head_cols], zs.at[0], zr.at[0], (section, target)
        ).start()
        return carry

    lax.fori_loop(1, REPLICAS, send_head, 0)
    pltpu.make_async_copy(tile_h.at[replica], hr.at[head_class, :, head_cols], zr.at[0]).start()

    @pl.when(c == 1)
    def _():
        for h in range(2):
            near_copy(h).wait_recv()

    for h in range(2):
        for slot in range(3):
            far_copy(1, slot, 0, h).wait_recv()
    out_grad[...] = (
        rs0[...] + rs[0].astype(f32) + rs[1].astype(f32) + rs[2].astype(f32)
    )
    pltpu.make_async_copy(er, er, erv.at[0]).wait()
    embed_grad[...] = er[0] + er[1] + er[2] + er[3]
    pltpu.make_async_copy(hr, hr, zr.at[0]).wait()
    head_grad[...] = hr[0] + hr[1] + hr[2] + hr[3]

    copies = [*mix_xl, *head_sends.values(), *forwards.values()]
    copies += [cot_all[j, part] for j in range(1, 8) for part in range(2)]
    copies += [hid_all[j] for j in range(1, 8)]
    copies += mix_core + mix_z + mix_diag + core_z + core_diag + ids_sends + log_far + log_core
    for copy in copies:
        copy.wait_send()
    for copies in (hid_sends, log_sends):
        for copy in copies[1:]:
            copy.wait_send()
    for m, copy in cot_sends:
        if m:
            copy.wait_send()

    @pl.when(root)
    def _():
        for j in range(1, 8):
            for copy in hidden_send(j):
                copy.wait_send()

    @pl.when(c == 0)
    def _():
        for h in range(2):
            far_copy(1, 1, 0, h).wait_send()
            far_copy(1, 1, 1, h).wait_send()
            near_copy(h).wait_send()

    @pl.when(c == 1)
    def _():
        for h in range(2):
            for part in range(2):
                for c_ in range(2):
                    far_copy(part, 0, c_, h).wait_send()

    sent = tile_e.at[pl.ds(0, REPLICAS - 1)]
    pltpu.make_async_copy(sent, sent, es.at[0]).wait()
    sent = tile_h.at[pl.ds(0, REPLICAS - 1)]
    pltpu.make_async_copy(sent, sent, zs.at[0]).wait()


def gradients(wide, mixed, head, weight, gain, target_ids, token_ids):
    dma = pltpu.SemaphoreType.DMA
    vm = pltpu.VMEM
    any_ = pl.BlockSpec(memory_space=pl.ANY)
    vmem = pl.BlockSpec(memory_space=pltpu.VMEM)
    return pl.pallas_call(
        kernel,
        out_shape=(
            jax.ShapeDtypeStruct((OWNED, WIDTH), f32),
            jax.ShapeDtypeStruct((8, WIDTH), f32),
            jax.ShapeDtypeStruct((8, WIDTH), f32),
        ),
        in_specs=[any_] * 4 + [vmem] * 3,
        out_specs=(vmem,) * 3,
        scratch_shapes=[
            vm((8, TOKENS, WIDTH), bf16),
            vm((SECTIONS, SLICE, WIDTH), bf16),
            vm((8, 256, WIDTH), bf16),
            vm((TOKENS, WIDTH), bf16),
            vm((TOKENS, WIDTH), f32),
            vm((TOKENS, WIDTH), bf16),
            vm((TOKENS, 128), f32),
            vm((BLOCK, WIDTH), bf16),
            vm((BLOCK, 128), f32),
            vm((BLOCK, VOCAB), f32),
            vm((BLOCK, VOCAB), bf16),
            vm((BLOCK, WIDTH), f32),
            vm((BLOCK, WIDTH), bf16),
            vm((8, BLOCK, 256), bf16),
            vm((8, TOKENS, 256), bf16),
            vm((8, BLOCK, 256), bf16),
            vm((8, TOKENS, 256), bf16),
            vm((8, TOKENS, SLICE), bf16),
            vm((8, 8, TOKENS), jnp.int32),
            vm((1, WIDTH), f32),
            vm((256, WIDTH), f32),
            vm((256, WIDTH), bf16),
            vm((3, OWNED, WIDTH), bf16),
            vm((OWNED, WIDTH), f32),
            vm((REPLICAS, 8, 256), f32),
            vm((REPLICAS, 8, 256), f32),
            vm((4, 8, WIDTH), f32),
            vm((4, 8, WIDTH), f32),
            dma((12,)),
            dma((2, 8)), dma((2, 8)),
            dma((8,)), dma((8,)),
            dma((8,)), dma((8,)),
            dma((8,)), dma((8,)),
            dma((2, 8)), dma((2,)),
            dma((8,)), dma((8,)),
            dma((8, 2)), dma((8, 2)),
            dma((2, 8)), dma((2, 8)),
            dma((8,)), dma((8,)),
            dma((8,)), dma((8,)),
            dma((8,)), dma((8,)),
            dma((2, 2, 2)), dma((2, 4)),
            dma((1,)), dma((1,)),
            dma((1,)), dma((1,)),
            dma((8, 4)), dma((8, 4)),
        ],
        compiler_params=pltpu.CompilerParams(
            collective_id=0, has_side_effects=True, vmem_limit_bytes=60 * 2**20
        ),
    )(wide, mixed, head, weight, gain, target_ids, token_ids)


def adam_update(master, first, second, gradient):
    first_next = beta_first * first + (1.0 - beta_first) * gradient
    second_next = beta_second * second + (1.0 - beta_second) * gradient * gradient
    master_next = master - learning_rate * (
        first_next / (jnp.sqrt(second_next) + adam_eps) + decay_rate * master
    )
    return (master_next, first_next, second_next)


def per_device(
    block_inputs, mixed_inputs, token_ids, target_ids, final_gain, out_weight, head_weight,
    out_master, out_first, out_second, head_master, head_first, head_second,
    embed_master, embed_first, embed_second,
):
    out_gradient, head_gradient, embed_gradient = gradients(
        block_inputs.reshape(TOKENS, WIDTH),
        mixed_inputs.reshape(TOKENS, WIDTH),
        head_weight,
        out_weight.reshape(WIDTH, WIDTH),
        final_gain,
        target_ids,
        token_ids,
    )
    return (
        *adam_update(out_master, out_first, out_second, out_gradient.reshape(out_master.shape)),
        *adam_update(head_master, head_first, head_second, head_gradient),
        *adam_update(embed_master, embed_first, embed_second, embed_gradient),
    )


def solution(mesh):
    tokens = P("section", None, "dp", None)
    rows = P("section", "dp", None)
    vocabulary = P(("section", "dp"), None)
    in_specs = (
        tokens, tokens, P(None, "dp"), P(None, "dp"), P(), P("section", None, None), P("section", None),
        rows, rows, rows, *(vocabulary,) * 6,
    )
    out_specs = (rows, rows, rows, *(vocabulary,) * 6)
    return jax.shard_map(
        per_device, mesh=mesh, in_specs=in_specs, out_specs=out_specs, check_vma=False
    )
```

```python
import jax
import jax.numpy as jnp
from jax import lax
from jax.experimental import pallas as pl
from jax.experimental.pallas import tpu as pltpu
from jax.sharding import PartitionSpec as P

norm_eps = 1e-05
beta_first = 0.9
beta_second = 0.95
adam_eps = 1e-05
learning_rate = 0.0003
decay_rate = 0.1
MESH = pl.DeviceIdType.MESH
bf16, f32 = jnp.bfloat16, jnp.float32
SECTIONS, REPLICAS = 8, 32
TOKENS, WIDTH, VOCAB = 256, 2048, 2048
BLOCK = TOKENS // SECTIONS
SLICE = VOCAB // SECTIONS
OWNED = 64
NT = (((1,), (1,)), ((), ()))
TN = (((0,), (0,)), ((), ()))


def dot(a, b, dims):
    return lax.dot_general(a, b, dims, preferred_element_type=f32)


def y_peer(y, k):
    return (y, y + 1 - 2 * (y % 2), (y + 2) % 4, 3 - y)[k]


def flip(value, k):
    return 1 - value if k else value


def kernel(
    wide_hbm, mixed_hbm, head_hbm, weight_hbm, gain_in, target_ids, token_ids,
    out_grad, head_grad, embed_grad,
    mix, hd, wbuf, wide, final, hid, stats, hmine, smine, lg, lcb, hc, cotb,
    gcot, bcot, ghid, bhid, alog, idsb, gain, psum, psend, rs, rs0, tile_e, tile_h, er, hr,
    loc, hs, hrv, fs, fr, ms, mr, ns, nr, ts, tr, ls, lr, gs, gr, cs, cr, is_, ir,
    vs, vr, ws, wr, rss, rsr, es, erv, zs, zr, fms, fmr,
):
    section = lax.axis_index("section")
    replica = lax.axis_index("dp")
    y, xh = section // 2, section % 2
    z, xl, c = replica // 4, (replica // 2) % 2, replica % 2
    sigma = 1 - 2 * (z % 2)
    root = section == SECTIONS - 1

    def dev(y_, xh_, z_, xl_, c_):
        return (y_ * 2 + xh_, z_ * 4 + xl_ * 2 + c_)

    def section_peer(j, cross=False):
        ky, kx = j // 2, j % 2
        return dev(y_peer(y, ky), flip(xh, kx), z, flip(xl, kx) if cross else xl, c)

    def member(m):
        kz, kl, kc = m // 4, (m // 2) % 2, m % 2
        return (z + 4 * kz) % 8, flip(xl, kl), flip(c, kc)

    def head_member(m):
        near = (z + (m // 2) % 2 * (1 - 2 * (z % 2))) % 8
        return (near + 4 * (m // 4)) % 8, xl, flip(c, m % 2)

    def head_column(z_, c_):
        return (z_ // 4) * 4 + (z_ % 2) * 2 + c_

    def remote(src, dst, send, recv, device):
        return pltpu.make_async_remote_copy(
            src_ref=src, dst_ref=dst, send_sem=send, recv_sem=recv,
            device_id=device, device_id_type=MESH,
        )

    load_mix = pltpu.make_async_copy(mixed_hbm, mix.at[0], loc.at[0])
    load_head = pltpu.make_async_copy(head_hbm, hd.at[section], loc.at[1])
    load_mix.start()
    load_head.start()
    load_wide = pltpu.make_async_copy(wide_hbm, wide, loc.at[2])

    def load_weight(n):
        return pltpu.make_async_copy(weight_hbm.at[pl.ds(n * 256, 256)], wbuf.at[n], loc.at[4 + n])

    @pl.when(root)
    def _():
        load_wide.start()
        for n in range(8):
            load_weight(n).start()

    barrier = pltpu.get_barrier_semaphore()
    for j in range(1, 8):
        pl.semaphore_signal(barrier, inc=1, device_id=section_peer(j), device_id_type=MESH)
        if j % 2:
            pl.semaphore_signal(barrier, inc=1, device_id=section_peer(j, True), device_id_type=MESH)

    def greet(k, carry):
        pl.semaphore_signal(
            barrier, inc=1, device_id=(section, (replica + k) % REPLICAS), device_id_type=MESH
        )
        return carry

    lax.fori_loop(1, REPLICAS, greet, 0)
    pl.semaphore_wait(barrier, 7 + 4 + REPLICAS - 1)

    half = pl.ds(pl.multiple_of(c * 128, 128), 128)
    def sender_slice(j):
        return y_peer(y, j // 2) * 2 + flip(xh, j % 2)

    HALVES = ((0, 64), (64, 128))
    head_sends = {}

    def head_copy(slot, source, peer, rows=(0, 128)):
        first, last = rows
        part = hd.at[
            sender_slice(source), pl.ds(pl.multiple_of(c * 128 + first, 16), last - first)
        ]
        lane = int(first > 0)
        return remote(part, part, hs.at[lane, slot], hrv.at[lane, slot], section_peer(peer, True))

    def head_send(slot, source, peer, rows=(0, 128)):
        copy = head_copy(slot, source, peer, rows)
        copy.start()
        head_sends[slot, rows] = copy

    load_head.wait()
    for j in (1, 2, 6):
        head_send(j, 0, j)
    load_mix.wait()
    partner = dev(y, xh, z, xl, 1 - c)

    def mix_copy(src, dst, device):
        return remote(mix.at[src], mix.at[dst], ms.at[dst], mr.at[dst], device)

    mix_xl = [
        remote(
            mix.at[0, pl.ds(h * 128, 128)], mix.at[2, pl.ds(h * 128, 128)],
            fms.at[1 + h, 0], fmr.at[1 + h, 0], dev(y, xh, z, 1 - xl, c),
        )
        for h in range(2)
    ]
    mix_core = [mix_copy(m, m + 1, partner) for m in (0, 2)]

    def far_mix(src, dst, device):
        rows = [pl.ds(k * 64, 64) for k in range(4)]
        return [
            remote(mix.at[src, r], mix.at[dst, r], fms.at[dst, k], fmr.at[dst, k], device)
            for k, r in enumerate(rows)
        ]

    mix_z = far_mix(0, 4, dev(y, xh, (z + 4) % 8, xl, c))
    mix_diag = far_mix(4, 6, dev(y, xh, z, 1 - xl, c))
    core_z = far_mix(4, 5, partner)
    core_diag = far_mix(6, 7, partner)
    mix_z[0].start()
    mix_z[1].start()
    mix_xl[0].start()
    mix_core[0].start()
    idsb[0] = jnp.broadcast_to(
        jnp.concatenate([token_ids[b : b + 1, :] for b in range(4)], axis=1), (8, TOKENS)
    )
    gain[...] = gain_in[...].reshape(1, WIDTH)
    ids_sends = []
    for m in range(1, 8):
        copy = remote(idsb.at[0], idsb.at[m], is_.at[m], ir.at[m], dev(y, xh, *member(m)))
        copy.start()
        ids_sends.append(copy)

    def hidden_send(j):
        ky, kx = j // 2, j % 2
        peer = section_peer(j)
        rows = pl.ds(pl.multiple_of(peer[0] * BLOCK, BLOCK), BLOCK)
        return (
            remote(hid.at[rows], hmine, ts.at[0, j], tr.at[0], peer),
            remote(stats.at[rows], smine, ts.at[1, j], tr.at[1], peer),
        )

    @pl.when(root)
    def _():
        load_wide.wait()
        for n in range(8):
            load_weight(n).wait()

        def columns(n, carry):
            cols = pl.ds(pl.multiple_of(n * 256, 256), 256)
            final[:, cols] = dot(mix[0], wbuf[n], NT) + wide[:, cols].astype(f32)
            return carry

        lax.fori_loop(0, 8, columns, 0)

        def norm(b, carry):
            rows = pl.ds(pl.multiple_of(b * BLOCK, BLOCK), BLOCK)
            values = final[rows, :]
            inverse = lax.rsqrt(jnp.mean(values * values, axis=-1, keepdims=True) + norm_eps)
            hid[rows, :] = (values * inverse * gain[...]).astype(bf16)
            stats[rows, :] = jnp.broadcast_to(inverse, (BLOCK, 128))
            return carry

        lax.fori_loop(0, SECTIONS, norm, 0)
        for j in (4, 5, 1, 3, 7, 2, 6):
            for copy in hidden_send(j):
                copy.start()
        hmine[...] = hid[(SECTIONS - 1) * BLOCK :, :]
        smine[...] = stats[(SECTIONS - 1) * BLOCK :, :]

    for rows in HALVES:
        head_send(4, 0, 4, rows)
    mix_xl[1].start()

    forwards = {}

    SPLIT = ((0, 112), (112, 128))

    def pass_on(j):
        part = hd.at[sender_slice(j), half]
        for rows in {3: SPLIT, 7: SPLIT, 4: HALVES, 5: HALVES}.get(j, ((0, 128),)):
            head_copy(j, j, j, rows).wait_recv()
            if j == 4:
                head_send(5, 4, 1, rows)
        copy = remote(part, part, fs.at[j], fr.at[j], partner)
        copy.start()
        forwards[j] = copy

    def pass_far(k):
        mix_z[k].wait_recv()
        mix_diag[k].start()
        core_z[k].start()
        if k == 0:
            mix_z[2].start()

    pass_on(1)
    head_send(3, 1, 2, SPLIT[0])
    head_send(7, 1, 6, SPLIT[0])
    pass_on(2)
    head_send(3, 2, 1, SPLIT[1])
    pass_on(6)
    head_send(7, 6, 1, SPLIT[1])
    pass_far(0)
    pass_on(4)

    @pl.when(jnp.logical_not(root))
    def _():
        for copy in hidden_send(1):
            copy.wait_recv()

    mine = pl.ds(pl.multiple_of(section * BLOCK, BLOCK), BLOCK)
    hid_sends = []
    for m in range(8):
        z_, xl_, c_ = head_member(m)
        block = head_column(z_, c_)
        src = hmine.at[:, pl.ds(pl.multiple_of(block * 256, 256), 256)]
        if m == 0:
            copy = pltpu.make_async_copy(src, ghid.at[0], nr.at[0])
        else:
            copy = remote(src, ghid.at[m], ns.at[m], nr.at[m], dev(y, xh, z_, xl_, c_))
        copy.start()
        hid_sends.append(copy)
    mix_z[3].start()

    def logits(j):
        n = sender_slice(j)
        lg[:, pl.ds(pl.multiple_of(n * SLICE, SLICE), SLICE)] = dot(hmine[...], hd[n], NT)

    for j in (0, 1, 2, 6):
        if j:
            forwards[j].wait_recv()
        logits(j)
    pass_far(1)
    for j in (3, 7, 5):
        pass_on(j)
    for j in (4, 3, 7, 5):
        forwards[j].wait_recv()
        logits(j)
    values = lg[...]
    shifted = jnp.exp(values - jnp.max(values, axis=1, keepdims=True))
    predicted = shifted / jnp.sum(shifted, axis=1, keepdims=True)
    columns_ = lax.broadcasted_iota(jnp.int32, (BLOCK, VOCAB), 1)
    batch_row = target_ids[pl.ds(section // 2, 1), :].astype(f32)
    lanes = lax.broadcasted_iota(jnp.int32, (BLOCK, 64), 1)
    places = lax.broadcasted_iota(jnp.int32, (BLOCK, 64), 0) + (section % 2) * BLOCK
    targets = jnp.sum(
        jnp.where(lanes == places, jnp.broadcast_to(batch_row, (BLOCK, 64)), 0.0), axis=1, keepdims=True
    )
    lcb[...] = jnp.where(targets == columns_.astype(f32), predicted - 1.0, predicted).astype(bf16)

    log_sends = []
    for j in range(8):
        peer_section = sender_slice(j)
        src = lcb.at[:, pl.ds(pl.multiple_of(peer_section * SLICE, SLICE), SLICE)]
        dst = alog.at[0, mine]
        if j == 0:
            copy = pltpu.make_async_copy(src, dst, lr.at[0])
        else:
            copy = remote(src, dst, ls.at[j], lr.at[j], section_peer(j))
        copy.start()
        log_sends.append(copy)

    def block_rows(j):
        return pl.ds(pl.multiple_of(sender_slice(j) * BLOCK, BLOCK), BLOCK)

    for n, copy in enumerate(hid_sends):
        if n == 0:
            copy.wait()
        else:
            copy.wait_recv()

    hid_all = {}

    def gather_hidden(slot, src, rows, peer):
        dst = bhid.at[:, rows]
        if slot == 0:
            copy = pltpu.make_async_copy(src, dst, wr.at[0])
        else:
            copy = remote(src, dst, ws.at[slot], wr.at[slot], section_peer(peer))
        copy.start()
        hid_all[slot] = copy

    for j in (1, 2, 6, 4, 0):
        gather_hidden(j, ghid, mine, j)
    def back(n, carry):
        cols = pl.ds(pl.multiple_of(n * 256, 256), 256)
        total = jnp.zeros((BLOCK, 256), f32)
        for s in range(SECTIONS):
            total += jnp.dot(
                lcb[:, s * SLICE : (s + 1) * SLICE], hd[s, :, cols], preferred_element_type=f32
            )
        hc[:, cols] = total
        return carry

    lax.fori_loop(0, WIDTH // 256, back, 0)
    scaled = hc[...] * gain[...]
    unit = hmine[...].astype(f32) / gain[...]
    inverse = smine[:, :1]
    along = jnp.mean(scaled * unit, axis=-1, keepdims=True)
    cotb[...] = (inverse * (scaled - unit * along)).astype(bf16)

    def offset(c_, part):
        low = (0, 1)[part]
        high = (-1, 2)[part]
        return sigma * (low + (high - low) * c_)

    def column_block(z_, xl_, c_, part):
        return ((z_ + offset(c_, part) + 8) % 8) * 2 + xl_

    cot_sends = []
    for m in (4, 5, 6, 7, 2, 3, 1, 0):
        z_, xl_, c_ = member(m)
        for part in range(2):
            block = column_block(z_, xl_, c_, part)
            src = cotb.at[:, pl.ds(pl.multiple_of(block * 128, 128), 128)]
            dst = gcot.at[m, :, pl.ds(part * 128, 128)]
            if m == 0:
                copy = pltpu.make_async_copy(src, dst, gr.at[m, part])
            else:
                copy = remote(src, dst, gs.at[m, part], gr.at[m, part], dev(y, xh, z_, xl_, c_))
            copy.start()
            cot_sends.append((m, copy))

    cot_all = {}

    def gather_cotangent(slot, part, src, rows, peer):
        members = pl.ds(part * 4, 4)
        dst = bcot.at[members, rows]
        if slot == 0:
            copy = pltpu.make_async_copy(src.at[members], dst, cr.at[part, 0])
        else:
            copy = remote(
                src.at[members, rows] if src is bcot else src.at[members],
                dst, cs.at[part, slot], cr.at[part, slot], section_peer(peer),
            )
        copy.start()
        cot_all[slot, part] = copy

    for part in range(2):
        for m, copy in cot_sends:
            if m // 4 == part:
                copy.wait() if m == 0 else copy.wait_recv()
        for j in (1, 2, 6, 4, 0):
            gather_cotangent(j, part, gcot, mine, j)

    pass_far(2)
    for part in range(2):
        cot_all[1, part].wait_recv()
        for j in (2, 6, 4):
            gather_cotangent(j + 1, part, bcot, block_rows(1), j)

    pass_far(3)
    hid_all[1].wait_recv()
    for j in (2, 6, 4):
        gather_hidden(j + 1, bhid.at[:, block_rows(1)], block_rows(1), j)
    for j, copy in enumerate(log_sends):
        if j == 0:
            copy.wait()
        else:
            copy.wait_recv()
    def log_copy(src, dst, device):
        return remote(alog.at[src], alog.at[dst], vs.at[dst], vr.at[dst], device)

    log_far = [log_copy(0, m, dev(y, xh, *head_member(m))) for m in (4, 6, 2)]
    log_core = [log_copy(m, m + 1, partner) for m in (0, 2, 4, 6)]
    for copy in log_far + log_core[:1]:
        copy.start()

    for h in range(2):
        mix_xl[h].wait_recv()
    mix_core[1].start()
    def pass_diag(k):
        mix_diag[k].wait_recv()
        core_diag[k].start()

    for k in range(3):
        pass_diag(k)
    for copy in mix_core:
        copy.wait_recv()

    def cotangent_part(part):
        cot_all[0, part].wait()
        for j in (2, 6, 4, 3, 7, 5):
            cot_all[j, part].wait_recv()

    def near_product(n, carry):
        cols = pl.ds(pl.multiple_of(n * 256, 256), 256)
        total = jnp.zeros((256, 256), f32)
        for m in range(4):
            total += dot(bcot[m], mix[m, :, cols], TN)
        psum[:, cols] = total
        return carry

    cotangent_part(0)
    lax.fori_loop(0, WIDTH // 256, near_product, 0)
    pass_diag(3)
    for copy in core_z + core_diag:
        copy.wait_recv()
    for copy in ids_sends:
        copy.wait_recv()
    cotangent_part(1)

    rows_ = section * SLICE + lax.broadcasted_iota(jnp.int32, (SLICE, TOKENS), 0)
    embed = jnp.zeros((SLICE, 256), f32)
    for m in range(8):
        marks = (idsb[m, :1, :] == rows_).astype(f32).astype(bf16)
        embed += jnp.dot(marks, bcot[m], preferred_element_type=f32)
    tile_e[...] = embed.reshape(REPLICAS, 8, 256)

    def send_embed(k, carry):
        target = (replica + k) % REPLICAS
        remote(
            tile_e.at[target], er.at[replica], es.at[0], erv.at[0], (section, target)
        ).start()
        return carry

    lax.fori_loop(1, REPLICAS, send_embed, 0)
    pltpu.make_async_copy(tile_e.at[replica], er.at[replica], erv.at[0]).start()

    def product(n, carry):
        cols = pl.ds(pl.multiple_of(n * 256, 256), 256)
        total = psum[:, cols]
        for m in range(4, 8):
            total += dot(bcot[m], mix[m, :, cols], TN)
        psum[:, cols] = total
        psend[:, cols] = total.astype(bf16)
        return carry

    def owner(part, c_):
        return dev(y, xh, (z + offset(c, part) + 8) % 8, xl, c_)

    def partial_rows(part, c_):
        return pl.ds((part * 2 + c_) * OWNED, OWNED)

    def far_copy(part, slot, c_, h):
        cols = pl.ds(h * (WIDTH // 2), WIDTH // 2)
        return remote(
            psend.at[partial_rows(part, c_), cols], rs.at[slot, :, cols],
            rss.at[h, part, c_], rsr.at[h, slot], owner(part, c_),
        )

    def near_copy(h):
        cols = pl.ds(h * (WIDTH // 2), WIDTH // 2)
        return remote(
            psum.at[partial_rows(0, 1), cols], rs0.at[:, cols], rss.at[h, 0, 1], rsr.at[h, 3], partner
        )

    for h in range(2):
        lax.fori_loop(h * 4, h * 4 + 4, product, 0)

        @pl.when(c == 0)
        def _(h=h):
            far_copy(1, 1, 0, h).start()
            far_copy(1, 1, 1, h).start()
            near_copy(h).start()

        @pl.when(c == 1)
        def _(h=h):
            far_copy(1, 2, 0, h).start()
            far_copy(1, 2, 1, h).start()
            far_copy(0, 0, 0, h).start()
            far_copy(0, 0, 1, h).start()

    @pl.when(c == 0)
    def _():
        rs0[...] = psum[:OWNED, :]

    for copy in log_far:
        copy.wait_recv()
    for copy in log_core[1:]:
        copy.start()
    for copy in log_core:
        copy.wait_recv()
    hid_all[0].wait()
    for j in (2, 6, 4, 3, 7, 5):
        hid_all[j].wait_recv()

    head = jnp.zeros((SLICE, 256), f32)
    for m in range(8):
        head += dot(alog[m], bhid[m], TN)
    tile_h[...] = head.reshape(REPLICAS, 8, 256)
    head_cols = pl.ds(pl.multiple_of(head_column(z, c) * 256, 256), 256)
    head_class = xl * 2 + (z // 2) % 2

    def send_head(k, carry):
        target = (replica + k) % REPLICAS
        remote(
            tile_h.at[target], hr.at[head_class, :, head_cols], zs.at[0], zr.at[0], (section, target)
        ).start()
        return carry

    lax.fori_loop(1, REPLICAS, send_head, 0)
    pltpu.make_async_copy(tile_h.at[replica], hr.at[head_class, :, head_cols], zr.at[0]).start()

    @pl.when(c == 1)
    def _():
        for h in range(2):
            near_copy(h).wait_recv()

    for h in range(2):
        for slot in range(3):
            far_copy(1, slot, 0, h).wait_recv()
    out_grad[...] = (
        rs0[...] + rs[0].astype(f32) + rs[1].astype(f32) + rs[2].astype(f32)
    )
    pltpu.make_async_copy(er, er, erv.at[0]).wait()
    for block in range(16):
        parts = [
            er[z_ * 4 + block % 2 * 2 + c_, :, part * 128 : (part + 1) * 128]
            for z_ in range(8)
            for c_ in range(2)
            for part in range(2)
            if (z_ + (1 - 2 * (z_ % 2)) * ((0, 1), (-1, 2))[c_][part]) % 8 == block // 2
        ]
        embed_grad[:, block * 128 : (block + 1) * 128] = (parts[0] + parts[1]) + (parts[2] + parts[3])
    pltpu.make_async_copy(hr, hr, zr.at[0]).wait()
    head_grad[...] = hr[0] + hr[1] + hr[2] + hr[3]

    copies = [*mix_xl, *head_sends.values(), *forwards.values()]
    copies += [cot_all[j, part] for j in range(1, 8) for part in range(2)]
    copies += [hid_all[j] for j in range(1, 8)]
    copies += mix_core + mix_z + mix_diag + core_z + core_diag + ids_sends + log_far + log_core
    for copy in copies:
        copy.wait_send()
    for copies in (hid_sends, log_sends):
        for copy in copies[1:]:
            copy.wait_send()
    for m, copy in cot_sends:
        if m:
            copy.wait_send()

    @pl.when(root)
    def _():
        for j in range(1, 8):
            for copy in hidden_send(j):
                copy.wait_send()

    @pl.when(c == 0)
    def _():
        for h in range(2):
            far_copy(1, 1, 0, h).wait_send()
            far_copy(1, 1, 1, h).wait_send()
            near_copy(h).wait_send()

    @pl.when(c == 1)
    def _():
        for h in range(2):
            for part in range(2):
                for c_ in range(2):
                    far_copy(part, 0, c_, h).wait_send()

    sent = tile_e.at[pl.ds(0, REPLICAS - 1)]
    pltpu.make_async_copy(sent, sent, es.at[0]).wait()
    sent = tile_h.at[pl.ds(0, REPLICAS - 1)]
    pltpu.make_async_copy(sent, sent, zs.at[0]).wait()


def gradients(wide, mixed, head, weight, gain, target_ids, token_ids):
    dma = pltpu.SemaphoreType.DMA
    vm = pltpu.VMEM
    any_ = pl.BlockSpec(memory_space=pl.ANY)
    vmem = pl.BlockSpec(memory_space=pltpu.VMEM)
    return pl.pallas_call(
        kernel,
        out_shape=(
            jax.ShapeDtypeStruct((OWNED, WIDTH), f32),
            jax.ShapeDtypeStruct((8, WIDTH), f32),
            jax.ShapeDtypeStruct((8, WIDTH), f32),
        ),
        in_specs=[any_] * 4 + [vmem] * 3,
        out_specs=(vmem,) * 3,
        scratch_shapes=[
            vm((8, TOKENS, WIDTH), bf16),
            vm((SECTIONS, SLICE, WIDTH), bf16),
            vm((8, 256, WIDTH), bf16),
            vm((TOKENS, WIDTH), bf16),
            vm((TOKENS, WIDTH), f32),
            vm((TOKENS, WIDTH), bf16),
            vm((TOKENS, 128), f32),
            vm((BLOCK, WIDTH), bf16),
            vm((BLOCK, 128), f32),
            vm((BLOCK, VOCAB), f32),
            vm((BLOCK, VOCAB), bf16),
            vm((BLOCK, WIDTH), f32),
            vm((BLOCK, WIDTH), bf16),
            vm((8, BLOCK, 256), bf16),
            vm((8, TOKENS, 256), bf16),
            vm((8, BLOCK, 256), bf16),
            vm((8, TOKENS, 256), bf16),
            vm((8, TOKENS, SLICE), bf16),
            vm((8, 8, TOKENS), jnp.int32),
            vm((1, WIDTH), f32),
            vm((256, WIDTH), f32),
            vm((256, WIDTH), bf16),
            vm((3, OWNED, WIDTH), bf16),
            vm((OWNED, WIDTH), f32),
            vm((REPLICAS, 8, 256), f32),
            vm((REPLICAS, 8, 256), f32),
            vm((REPLICAS, 8, 256), f32),
            vm((4, 8, WIDTH), f32),
            dma((12,)),
            dma((2, 8)), dma((2, 8)),
            dma((8,)), dma((8,)),
            dma((8,)), dma((8,)),
            dma((8,)), dma((8,)),
            dma((2, 8)), dma((2,)),
            dma((8,)), dma((8,)),
            dma((8, 2)), dma((8, 2)),
            dma((2, 8)), dma((2, 8)),
            dma((8,)), dma((8,)),
            dma((8,)), dma((8,)),
            dma((8,)), dma((8,)),
            dma((2, 2, 2)), dma((2, 4)),
            dma((1,)), dma((1,)),
            dma((1,)), dma((1,)),
            dma((8, 4)), dma((8, 4)),
        ],
        compiler_params=pltpu.CompilerParams(
            collective_id=0, has_side_effects=True, vmem_limit_bytes=60 * 2**20
        ),
    )(wide, mixed, head, weight, gain, target_ids, token_ids)


def adam_update(master, first, second, gradient):
    first_next = beta_first * first + (1.0 - beta_first) * gradient
    second_next = beta_second * second + (1.0 - beta_second) * gradient * gradient
    master_next = master - learning_rate * (
        first_next / (jnp.sqrt(second_next) + adam_eps) + decay_rate * master
    )
    return (master_next, first_next, second_next)


def adam_kernel(*refs):
    def update(k, rows):
        gradient, master, first, second = (refs[4 * k + n][rows, :] for n in range(4))
        results = adam_update(master, first, second, gradient)
        for n in range(3):
            refs[12 + 3 * k + n][rows, :] = results[n]

    def chunk(i, carry):
        update(0, pl.ds(pl.multiple_of(i * 8, 8), 8))
        return carry

    lax.fori_loop(0, refs[0].shape[0] // 8, chunk, 0)

    @pl.when(pl.program_id(0) == 0)
    def _():
        update(1, slice(None))
        update(2, slice(None))


def adam(groups):
    steps = 2
    wide = pl.BlockSpec((OWNED // steps, WIDTH), lambda i: (i, 0))
    narrow = pl.BlockSpec((8, WIDTH), lambda i: (0, 0))
    specs = [wide] * 4 + [narrow] * 8
    operands = [array for group in groups for array in group]
    return pl.pallas_call(
        adam_kernel,
        out_shape=[jax.ShapeDtypeStruct(groups[k][0].shape, f32) for k in range(3) for _ in range(3)],
        grid=(steps,),
        in_specs=specs,
        out_specs=[wide] * 3 + [narrow] * 6,
    )(*operands)


def per_device(
    block_inputs, mixed_inputs, token_ids, target_ids, final_gain, out_weight, head_weight,
    out_master, out_first, out_second, head_master, head_first, head_second,
    embed_master, embed_first, embed_second,
):
    out_gradient, head_gradient, embed_gradient = gradients(
        block_inputs.reshape(TOKENS, WIDTH),
        mixed_inputs.reshape(TOKENS, WIDTH),
        head_weight,
        out_weight.reshape(WIDTH, WIDTH),
        final_gain,
        target_ids,
        token_ids,
    )
    shape = out_master.shape
    flat = (OWNED, WIDTH)
    results = adam(
        (
            (out_gradient, out_master.reshape(flat), out_first.reshape(flat), out_second.reshape(flat)),
            (head_gradient, head_master, head_first, head_second),
            (embed_gradient, embed_master, embed_first, embed_second),
        )
    )
    return (*(value.reshape(shape) for value in results[:3]), *results[3:])


def solution(mesh):
    tokens = P("section", None, "dp", None)
    rows = P("section", "dp", None)
    vocabulary = P(("section", "dp"), None)
    in_specs = (
        tokens, tokens, P(None, "dp"), P(None, "dp"), P(), P("section", None, None), P("section", None),
        rows, rows, rows, *(vocabulary,) * 6,
    )
    out_specs = (rows, rows, rows, *(vocabulary,) * 6)
    return jax.shard_map(
        per_device, mesh=mesh, in_specs=in_specs, out_specs=out_specs, check_vma=False
    )
```

```python
import jax
import jax.numpy as jnp
from jax import lax
from jax.experimental import pallas as pl
from jax.experimental.pallas import tpu as pltpu
from jax.sharding import PartitionSpec as P

norm_eps = 1e-05
beta_first = 0.9
beta_second = 0.95
adam_eps = 1e-05
learning_rate = 0.0003
decay_rate = 0.1
MESH = pl.DeviceIdType.MESH
bf16, f32 = jnp.bfloat16, jnp.float32
SECTIONS, REPLICAS = 8, 32
TOKENS, WIDTH, VOCAB = 256, 2048, 2048
BLOCK = TOKENS // SECTIONS
SLICE = VOCAB // SECTIONS
OWNED = 64
NT = (((1,), (1,)), ((), ()))
TN = (((0,), (0,)), ((), ()))


def dot(a, b, dims):
    return lax.dot_general(a, b, dims, preferred_element_type=f32)


def y_peer(y, k):
    return (y, y + 1 - 2 * (y % 2), (y + 2) % 4, 3 - y)[k]


def flip(value, k):
    return 1 - value if k else value


def kernel(
    wide_hbm, mixed_hbm, head_hbm, weight_hbm, gain_in, target_ids, token_ids,
    out_grad, head_grad, embed_grad,
    mix, hd, wbuf, wide, final, hid, stats, hmine, smine, lg, lcb, hc, cotb,
    gcot, bcot, ghid, bhid, alog, idsb, gain, psum, psend, rs, rs0, tile_e, tile_h, er, hr,
    loc, hs, hrv, fs, fr, ms, mr, ns, nr, ts, tr, ls, lr, gs, gr, cs, cr, is_, ir,
    vs, vr, ws, wr, rss, rsr, es, erv, zs, zr, fms, fmr,
):
    section = lax.axis_index("section")
    replica = lax.axis_index("dp")
    y, xh = section // 2, section % 2
    z, xl, c = replica // 4, (replica // 2) % 2, replica % 2
    sigma = 1 - 2 * (z % 2)
    root = section == SECTIONS - 1

    def dev(y_, xh_, z_, xl_, c_):
        return (y_ * 2 + xh_, z_ * 4 + xl_ * 2 + c_)

    def section_peer(j, cross=False):
        ky, kx = j // 2, j % 2
        return dev(y_peer(y, ky), flip(xh, kx), z, flip(xl, kx) if cross else xl, c)

    def member(m):
        kz, kl, kc = m // 4, (m // 2) % 2, m % 2
        return (z + 4 * kz) % 8, flip(xl, kl), flip(c, kc)

    def head_member(m):
        near = (z + (m // 2) % 2 * (1 - 2 * (z % 2))) % 8
        return (near + 4 * (m // 4)) % 8, xl, flip(c, m % 2)

    def head_column(z_, c_):
        return (z_ // 4) * 4 + (z_ % 2) * 2 + c_

    def remote(src, dst, send, recv, device):
        return pltpu.make_async_remote_copy(
            src_ref=src, dst_ref=dst, send_sem=send, recv_sem=recv,
            device_id=device, device_id_type=MESH,
        )

    load_mix = pltpu.make_async_copy(mixed_hbm, mix.at[0], loc.at[0])
    load_head = pltpu.make_async_copy(head_hbm, hd.at[section], loc.at[1])
    load_mix.start()
    load_head.start()
    load_wide = pltpu.make_async_copy(wide_hbm, wide, loc.at[2])

    def load_weight(n):
        return pltpu.make_async_copy(weight_hbm.at[pl.ds(n * 256, 256)], wbuf.at[n], loc.at[4 + n])

    @pl.when(root)
    def _():
        load_wide.start()
        for n in range(8):
            load_weight(n).start()

    barrier = pltpu.get_barrier_semaphore()
    for j in range(1, 8):
        pl.semaphore_signal(barrier, inc=1, device_id=section_peer(j), device_id_type=MESH)
        if j % 2:
            pl.semaphore_signal(barrier, inc=1, device_id=section_peer(j, True), device_id_type=MESH)

    def greet(k, carry):
        pl.semaphore_signal(
            barrier, inc=1, device_id=(section, (replica + k) % REPLICAS), device_id_type=MESH
        )
        return carry

    lax.fori_loop(1, REPLICAS, greet, 0)
    pl.semaphore_wait(barrier, 7 + 4 + REPLICAS - 1)

    half = pl.ds(pl.multiple_of(c * 128, 128), 128)
    def sender_slice(j):
        return y_peer(y, j // 2) * 2 + flip(xh, j % 2)

    HALVES = ((0, 64), (64, 128))
    head_sends = {}

    def head_copy(slot, source, peer, rows=(0, 128)):
        first, last = rows
        part = hd.at[
            sender_slice(source), pl.ds(pl.multiple_of(c * 128 + first, 16), last - first)
        ]
        lane = int(first > 0)
        return remote(part, part, hs.at[lane, slot], hrv.at[lane, slot], section_peer(peer, True))

    def head_send(slot, source, peer, rows=(0, 128)):
        copy = head_copy(slot, source, peer, rows)
        copy.start()
        head_sends[slot, rows] = copy

    load_head.wait()
    for j in (1, 2, 6):
        head_send(j, 0, j)
    load_mix.wait()
    partner = dev(y, xh, z, xl, 1 - c)

    def mix_copy(src, dst, device):
        return remote(mix.at[src], mix.at[dst], ms.at[dst], mr.at[dst], device)

    mix_xl = [
        remote(
            mix.at[0, pl.ds(h * 128, 128)], mix.at[2, pl.ds(h * 128, 128)],
            fms.at[1 + h, 0], fmr.at[1 + h, 0], dev(y, xh, z, 1 - xl, c),
        )
        for h in range(2)
    ]
    mix_core = [mix_copy(m, m + 1, partner) for m in (0, 2)]

    def far_mix(src, dst, device):
        rows = [pl.ds(k * 64, 64) for k in range(4)]
        return [
            remote(mix.at[src, r], mix.at[dst, r], fms.at[dst, k], fmr.at[dst, k], device)
            for k, r in enumerate(rows)
        ]

    mix_z = far_mix(0, 4, dev(y, xh, (z + 4) % 8, xl, c))
    mix_diag = far_mix(4, 6, dev(y, xh, z, 1 - xl, c))
    core_z = far_mix(4, 5, partner)
    core_diag = far_mix(6, 7, partner)
    mix_z[0].start()
    mix_z[1].start()
    mix_xl[0].start()
    mix_core[0].start()
    idsb[0] = jnp.broadcast_to(
        jnp.concatenate([token_ids[b : b + 1, :] for b in range(4)], axis=1), (8, TOKENS)
    )
    gain[...] = gain_in[...].reshape(1, WIDTH)
    ids_sends = []
    for m in range(1, 8):
        copy = remote(idsb.at[0], idsb.at[m], is_.at[m], ir.at[m], dev(y, xh, *member(m)))
        copy.start()
        ids_sends.append(copy)

    def hidden_send(j):
        ky, kx = j // 2, j % 2
        peer = section_peer(j)
        rows = pl.ds(pl.multiple_of(peer[0] * BLOCK, BLOCK), BLOCK)
        return (
            remote(hid.at[rows], hmine, ts.at[0, j], tr.at[0], peer),
            remote(stats.at[rows], smine, ts.at[1, j], tr.at[1], peer),
        )

    @pl.when(root)
    def _():
        load_wide.wait()
        for n in range(8):
            load_weight(n).wait()

        def columns(n, carry):
            cols = pl.ds(pl.multiple_of(n * 256, 256), 256)
            final[:, cols] = dot(mix[0], wbuf[n], NT) + wide[:, cols].astype(f32)
            return carry

        lax.fori_loop(0, 8, columns, 0)

        def norm(b, carry):
            rows = pl.ds(pl.multiple_of(b * BLOCK, BLOCK), BLOCK)
            values = final[rows, :]
            inverse = lax.rsqrt(jnp.mean(values * values, axis=-1, keepdims=True) + norm_eps)
            hid[rows, :] = (values * inverse * gain[...]).astype(bf16)
            stats[rows, :] = jnp.broadcast_to(inverse, (BLOCK, 128))
            return carry

        lax.fori_loop(0, SECTIONS, norm, 0)
        for j in (4, 5, 1, 3, 7, 2, 6):
            for copy in hidden_send(j):
                copy.start()
        hmine[...] = hid[(SECTIONS - 1) * BLOCK :, :]
        smine[...] = stats[(SECTIONS - 1) * BLOCK :, :]

    for rows in HALVES:
        head_send(4, 0, 4, rows)
    mix_xl[1].start()

    forwards = {}

    SPLIT = ((0, 112), (112, 128))

    def pass_on(j):
        part = hd.at[sender_slice(j), half]
        for rows in {3: SPLIT, 7: SPLIT, 4: HALVES, 5: HALVES}.get(j, ((0, 128),)):
            head_copy(j, j, j, rows).wait_recv()
            if j == 4:
                head_send(5, 4, 1, rows)
        copy = remote(part, part, fs.at[j], fr.at[j], partner)
        copy.start()
        forwards[j] = copy

    def pass_far(k):
        mix_z[k].wait_recv()
        mix_diag[k].start()
        core_z[k].start()
        if k == 0:
            mix_z[2].start()

    pass_on(1)
    head_send(3, 1, 2, SPLIT[0])
    head_send(7, 1, 6, SPLIT[0])
    pass_on(2)
    head_send(3, 2, 1, SPLIT[1])
    pass_on(6)
    head_send(7, 6, 1, SPLIT[1])
    pass_far(0)
    pass_on(4)

    @pl.when(jnp.logical_not(root))
    def _():
        for copy in hidden_send(1):
            copy.wait_recv()

    mine = pl.ds(pl.multiple_of(section * BLOCK, BLOCK), BLOCK)
    hid_sends = []
    for m in range(8):
        z_, xl_, c_ = head_member(m)
        block = head_column(z_, c_)
        src = hmine.at[:, pl.ds(pl.multiple_of(block * 256, 256), 256)]
        if m == 0:
            copy = pltpu.make_async_copy(src, ghid.at[0], nr.at[0])
        else:
            copy = remote(src, ghid.at[m], ns.at[m], nr.at[m], dev(y, xh, z_, xl_, c_))
        copy.start()
        hid_sends.append(copy)
    mix_z[3].start()

    def logits(j):
        n = sender_slice(j)
        lg[:, pl.ds(pl.multiple_of(n * SLICE, SLICE), SLICE)] = dot(hmine[...], hd[n], NT)

    for j in (0, 1, 2, 6):
        if j:
            forwards[j].wait_recv()
        logits(j)
    pass_far(1)
    for j in (3, 7, 5):
        pass_on(j)
    for j in (4, 3, 7, 5):
        forwards[j].wait_recv()
        logits(j)
    values = lg[...]
    shifted = jnp.exp(values - jnp.max(values, axis=1, keepdims=True))
    predicted = shifted / jnp.sum(shifted, axis=1, keepdims=True)
    columns_ = lax.broadcasted_iota(jnp.int32, (BLOCK, VOCAB), 1)
    batch_row = target_ids[pl.ds(section // 2, 1), :].astype(f32)
    lanes = lax.broadcasted_iota(jnp.int32, (BLOCK, 64), 1)
    places = lax.broadcasted_iota(jnp.int32, (BLOCK, 64), 0) + (section % 2) * BLOCK
    targets = jnp.sum(
        jnp.where(lanes == places, jnp.broadcast_to(batch_row, (BLOCK, 64)), 0.0), axis=1, keepdims=True
    )
    lcb[...] = jnp.where(targets == columns_.astype(f32), predicted - 1.0, predicted).astype(bf16)

    log_sends = []
    for j in range(8):
        peer_section = sender_slice(j)
        src = lcb.at[:, pl.ds(pl.multiple_of(peer_section * SLICE, SLICE), SLICE)]
        dst = alog.at[0, mine]
        if j == 0:
            copy = pltpu.make_async_copy(src, dst, lr.at[0])
        else:
            copy = remote(src, dst, ls.at[j], lr.at[j], section_peer(j))
        copy.start()
        log_sends.append(copy)

    def block_rows(j):
        return pl.ds(pl.multiple_of(sender_slice(j) * BLOCK, BLOCK), BLOCK)

    for n, copy in enumerate(hid_sends):
        if n == 0:
            copy.wait()
        else:
            copy.wait_recv()

    hid_all = {}

    def gather_hidden(slot, src, rows, peer):
        dst = bhid.at[:, rows]
        if slot == 0:
            copy = pltpu.make_async_copy(src, dst, wr.at[0])
        else:
            copy = remote(src, dst, ws.at[slot], wr.at[slot], section_peer(peer))
        copy.start()
        hid_all[slot] = copy

    for j in (1, 2, 6, 4, 0):
        gather_hidden(j, ghid, mine, j)
    def back(n, carry):
        cols = pl.ds(pl.multiple_of(n * 256, 256), 256)
        total = jnp.zeros((BLOCK, 256), f32)
        for s in range(SECTIONS):
            total += jnp.dot(
                lcb[:, s * SLICE : (s + 1) * SLICE], hd[s, :, cols], preferred_element_type=f32
            )
        hc[:, cols] = total
        return carry

    lax.fori_loop(0, WIDTH // 256, back, 0)
    scaled = hc[...] * gain[...]
    unit = hmine[...].astype(f32) / gain[...]
    inverse = smine[:, :1]
    along = jnp.mean(scaled * unit, axis=-1, keepdims=True)
    cotb[...] = (inverse * (scaled - unit * along)).astype(bf16)

    def offset(c_, part):
        low = (0, 1)[part]
        high = (-1, 2)[part]
        return sigma * (low + (high - low) * c_)

    def column_block(z_, xl_, c_, part):
        return ((z_ + offset(c_, part) + 8) % 8) * 2 + xl_

    cot_sends = []
    for m in (4, 5, 6, 7, 2, 3, 1, 0):
        z_, xl_, c_ = member(m)
        for part in range(2):
            block = column_block(z_, xl_, c_, part)
            src = cotb.at[:, pl.ds(pl.multiple_of(block * 128, 128), 128)]
            dst = gcot.at[m, :, pl.ds(part * 128, 128)]
            if m == 0:
                copy = pltpu.make_async_copy(src, dst, gr.at[m, part])
            else:
                copy = remote(src, dst, gs.at[m, part], gr.at[m, part], dev(y, xh, z_, xl_, c_))
            copy.start()
            cot_sends.append((m, copy))

    cot_all = {}

    def gather_cotangent(slot, part, src, rows, peer):
        members = pl.ds(part * 4, 4)
        dst = bcot.at[members, rows]
        if slot == 0:
            copy = pltpu.make_async_copy(src.at[members], dst, cr.at[part, 0])
        else:
            copy = remote(
                src.at[members, rows] if src is bcot else src.at[members],
                dst, cs.at[part, slot], cr.at[part, slot], section_peer(peer),
            )
        copy.start()
        cot_all[slot, part] = copy

    for part in range(2):
        for m, copy in cot_sends:
            if m // 4 == part:
                copy.wait() if m == 0 else copy.wait_recv()
        for j in (1, 2, 6, 4, 0):
            gather_cotangent(j, part, gcot, mine, j)

    pass_far(2)
    for part in range(2):
        cot_all[1, part].wait_recv()
        for j in (2, 6, 4):
            gather_cotangent(j + 1, part, bcot, block_rows(1), j)

    pass_far(3)
    hid_all[1].wait_recv()
    for j in (2, 6, 4):
        gather_hidden(j + 1, bhid.at[:, block_rows(1)], block_rows(1), j)
    for j, copy in enumerate(log_sends):
        if j == 0:
            copy.wait()
        else:
            copy.wait_recv()
    def log_copy(src, dst, device):
        return remote(alog.at[src], alog.at[dst], vs.at[dst], vr.at[dst], device)

    log_far = [log_copy(0, m, dev(y, xh, *head_member(m))) for m in (4, 6, 2)]
    log_core = [log_copy(m, m + 1, partner) for m in (0, 2, 4, 6)]
    for copy in log_far + log_core[:1]:
        copy.start()

    for h in range(2):
        mix_xl[h].wait_recv()
    mix_core[1].start()
    def pass_diag(k):
        mix_diag[k].wait_recv()
        core_diag[k].start()

    for k in range(3):
        pass_diag(k)
    for copy in mix_core:
        copy.wait_recv()

    def cotangent_part(part):
        cot_all[0, part].wait()
        for j in (2, 6, 4, 3, 7, 5):
            cot_all[j, part].wait_recv()

    def near_product(n, carry):
        cols = pl.ds(pl.multiple_of(n * 256, 256), 256)
        total = jnp.zeros((256, 256), f32)
        for m in range(4):
            total += dot(bcot[m], mix[m, :, cols], TN)
        psum[:, cols] = total
        return carry

    def embed_part(part):
        rows_ = section * SLICE + lax.broadcasted_iota(jnp.int32, (SLICE, TOKENS), 0)
        embed = jnp.zeros((SLICE, 256), f32)
        for m in range(part * 4, part * 4 + 4):
            marks = (idsb[m, :1, :] == rows_).astype(f32).astype(bf16)
            embed += jnp.dot(marks, bcot[m], preferred_element_type=f32)
        return embed.reshape(REPLICAS, 8, 256)

    cotangent_part(0)
    lax.fori_loop(0, WIDTH // 256, near_product, 0)
    pass_diag(3)
    for copy in ids_sends:
        copy.wait_recv()
    tile_e[...] = embed_part(0)
    cotangent_part(1)
    tile_e[...] += embed_part(1)
    def send_embed(k, carry):
        target = (replica + k) % REPLICAS
        remote(
            tile_e.at[target], er.at[replica], es.at[0], erv.at[0], (section, target)
        ).start()
        return carry

    lax.fori_loop(1, REPLICAS, send_embed, 0)
    pltpu.make_async_copy(tile_e.at[replica], er.at[replica], erv.at[0]).start()

    for copy in core_z + core_diag:
        copy.wait_recv()

    def product(n, carry):
        cols = pl.ds(pl.multiple_of(n * 256, 256), 256)
        total = psum[:, cols]
        for m in range(4, 8):
            total += dot(bcot[m], mix[m, :, cols], TN)
        psum[:, cols] = total
        psend[:, cols] = total.astype(bf16)
        return carry

    def owner(part, c_):
        return dev(y, xh, (z + offset(c, part) + 8) % 8, xl, c_)

    def partial_rows(part, c_):
        return pl.ds((part * 2 + c_) * OWNED, OWNED)

    def far_copy(part, slot, c_, h):
        cols = pl.ds(h * (WIDTH // 2), WIDTH // 2)
        return remote(
            psend.at[partial_rows(part, c_), cols], rs.at[slot, :, cols],
            rss.at[h, part, c_], rsr.at[h, slot], owner(part, c_),
        )

    def near_copy(h):
        cols = pl.ds(h * (WIDTH // 2), WIDTH // 2)
        return remote(
            psum.at[partial_rows(0, 1), cols], rs0.at[:, cols], rss.at[h, 0, 1], rsr.at[h, 3], partner
        )

    for h in range(2):
        lax.fori_loop(h * 4, h * 4 + 4, product, 0)

        @pl.when(c == 0)
        def _(h=h):
            far_copy(1, 1, 0, h).start()
            far_copy(1, 1, 1, h).start()
            near_copy(h).start()

        @pl.when(c == 1)
        def _(h=h):
            far_copy(1, 2, 0, h).start()
            far_copy(1, 2, 1, h).start()
            far_copy(0, 0, 0, h).start()
            far_copy(0, 0, 1, h).start()

    @pl.when(c == 0)
    def _():
        rs0[...] = psum[:OWNED, :]

    for copy in log_far:
        copy.wait_recv()
    for copy in log_core[1:]:
        copy.start()
    for copy in log_core:
        copy.wait_recv()
    hid_all[0].wait()
    for j in (2, 6, 4, 3, 7, 5):
        hid_all[j].wait_recv()

    head = jnp.zeros((SLICE, 256), f32)
    for m in range(8):
        head += dot(alog[m], bhid[m], TN)
    tile_h[...] = head.reshape(REPLICAS, 8, 256)
    head_cols = pl.ds(pl.multiple_of(head_column(z, c) * 256, 256), 256)
    head_class = xl * 2 + (z // 2) % 2

    def send_head(k, carry):
        target = (replica + k) % REPLICAS
        remote(
            tile_h.at[target], hr.at[head_class, :, head_cols], zs.at[0], zr.at[0], (section, target)
        ).start()
        return carry

    lax.fori_loop(1, REPLICAS, send_head, 0)
    pltpu.make_async_copy(tile_h.at[replica], hr.at[head_class, :, head_cols], zr.at[0]).start()

    @pl.when(c == 1)
    def _():
        for h in range(2):
            near_copy(h).wait_recv()

    for h in range(2):
        for slot in range(3):
            far_copy(1, slot, 0, h).wait_recv()
    out_grad[...] = (
        rs0[...] + rs[0].astype(f32) + rs[1].astype(f32) + rs[2].astype(f32)
    )
    pltpu.make_async_copy(er, er, erv.at[0]).wait()
    for block in range(16):
        parts = [
            er[z_ * 4 + block % 2 * 2 + c_, :, part * 128 : (part + 1) * 128]
            for z_ in range(8)
            for c_ in range(2)
            for part in range(2)
            if (z_ + (1 - 2 * (z_ % 2)) * ((0, 1), (-1, 2))[c_][part]) % 8 == block // 2
        ]
        embed_grad[:, block * 128 : (block + 1) * 128] = (parts[0] + parts[1]) + (parts[2] + parts[3])
    pltpu.make_async_copy(hr, hr, zr.at[0]).wait()
    head_grad[...] = hr[0] + hr[1] + hr[2] + hr[3]

    copies = [*mix_xl, *head_sends.values(), *forwards.values()]
    copies += [cot_all[j, part] for j in range(1, 8) for part in range(2)]
    copies += [hid_all[j] for j in range(1, 8)]
    copies += mix_core + mix_z + mix_diag + core_z + core_diag + ids_sends + log_far + log_core
    for copy in copies:
        copy.wait_send()
    for copies in (hid_sends, log_sends):
        for copy in copies[1:]:
            copy.wait_send()
    for m, copy in cot_sends:
        if m:
            copy.wait_send()

    @pl.when(root)
    def _():
        for j in range(1, 8):
            for copy in hidden_send(j):
                copy.wait_send()

    @pl.when(c == 0)
    def _():
        for h in range(2):
            far_copy(1, 1, 0, h).wait_send()
            far_copy(1, 1, 1, h).wait_send()
            near_copy(h).wait_send()

    @pl.when(c == 1)
    def _():
        for h in range(2):
            for part in range(2):
                for c_ in range(2):
                    far_copy(part, 0, c_, h).wait_send()

    sent = tile_e.at[pl.ds(0, REPLICAS - 1)]
    pltpu.make_async_copy(sent, sent, es.at[0]).wait()
    sent = tile_h.at[pl.ds(0, REPLICAS - 1)]
    pltpu.make_async_copy(sent, sent, zs.at[0]).wait()


def gradients(wide, mixed, head, weight, gain, target_ids, token_ids):
    dma = pltpu.SemaphoreType.DMA
    vm = pltpu.VMEM
    any_ = pl.BlockSpec(memory_space=pl.ANY)
    vmem = pl.BlockSpec(memory_space=pltpu.VMEM)
    return pl.pallas_call(
        kernel,
        out_shape=(
            jax.ShapeDtypeStruct((OWNED, WIDTH), f32),
            jax.ShapeDtypeStruct((8, WIDTH), f32),
            jax.ShapeDtypeStruct((8, WIDTH), f32),
        ),
        in_specs=[any_] * 4 + [vmem] * 3,
        out_specs=(vmem,) * 3,
        scratch_shapes=[
            vm((8, TOKENS, WIDTH), bf16),
            vm((SECTIONS, SLICE, WIDTH), bf16),
            vm((8, 256, WIDTH), bf16),
            vm((TOKENS, WIDTH), bf16),
            vm((TOKENS, WIDTH), f32),
            vm((TOKENS, WIDTH), bf16),
            vm((TOKENS, 128), f32),
            vm((BLOCK, WIDTH), bf16),
            vm((BLOCK, 128), f32),
            vm((BLOCK, VOCAB), f32),
            vm((BLOCK, VOCAB), bf16),
            vm((BLOCK, WIDTH), f32),
            vm((BLOCK, WIDTH), bf16),
            vm((8, BLOCK, 256), bf16),
            vm((8, TOKENS, 256), bf16),
            vm((8, BLOCK, 256), bf16),
            vm((8, TOKENS, 256), bf16),
            vm((8, TOKENS, SLICE), bf16),
            vm((8, 8, TOKENS), jnp.int32),
            vm((1, WIDTH), f32),
            vm((256, WIDTH), f32),
            vm((256, WIDTH), bf16),
            vm((3, OWNED, WIDTH), bf16),
            vm((OWNED, WIDTH), f32),
            vm((REPLICAS, 8, 256), f32),
            vm((REPLICAS, 8, 256), f32),
            vm((REPLICAS, 8, 256), f32),
            vm((4, 8, WIDTH), f32),
            dma((12,)),
            dma((2, 8)), dma((2, 8)),
            dma((8,)), dma((8,)),
            dma((8,)), dma((8,)),
            dma((8,)), dma((8,)),
            dma((2, 8)), dma((2,)),
            dma((8,)), dma((8,)),
            dma((8, 2)), dma((8, 2)),
            dma((2, 8)), dma((2, 8)),
            dma((8,)), dma((8,)),
            dma((8,)), dma((8,)),
            dma((8,)), dma((8,)),
            dma((2, 2, 2)), dma((2, 4)),
            dma((1,)), dma((1,)),
            dma((1,)), dma((1,)),
            dma((8, 4)), dma((8, 4)),
        ],
        compiler_params=pltpu.CompilerParams(
            collective_id=0, has_side_effects=True, vmem_limit_bytes=60 * 2**20
        ),
    )(wide, mixed, head, weight, gain, target_ids, token_ids)


def adam_update(master, first, second, gradient):
    first_next = beta_first * first + (1.0 - beta_first) * gradient
    second_next = beta_second * second + (1.0 - beta_second) * gradient * gradient
    master_next = master - learning_rate * (
        first_next / (jnp.sqrt(second_next) + adam_eps) + decay_rate * master
    )
    return (master_next, first_next, second_next)


def adam_kernel(*refs):
    def update(k, rows):
        gradient, master, first, second = (refs[4 * k + n][rows, :] for n in range(4))
        results = adam_update(master, first, second, gradient)
        for n in range(3):
            refs[12 + 3 * k + n][rows, :] = results[n]

    def chunk(i, carry):
        update(0, pl.ds(pl.multiple_of(i * 8, 8), 8))
        return carry

    lax.fori_loop(0, refs[0].shape[0] // 8, chunk, 0)

    @pl.when(pl.program_id(0) == 0)
    def _():
        update(1, slice(None))
        update(2, slice(None))


def adam(groups):
    steps = 2
    wide = pl.BlockSpec((OWNED // steps, WIDTH), lambda i: (i, 0))
    narrow = pl.BlockSpec((8, WIDTH), lambda i: (0, 0))
    specs = [wide] * 4 + [narrow] * 8
    operands = [array for group in groups for array in group]
    return pl.pallas_call(
        adam_kernel,
        out_shape=[jax.ShapeDtypeStruct(groups[k][0].shape, f32) for k in range(3) for _ in range(3)],
        grid=(steps,),
        in_specs=specs,
        out_specs=[wide] * 3 + [narrow] * 6,
    )(*operands)


def per_device(
    block_inputs, mixed_inputs, token_ids, target_ids, final_gain, out_weight, head_weight,
    out_master, out_first, out_second, head_master, head_first, head_second,
    embed_master, embed_first, embed_second,
):
    out_gradient, head_gradient, embed_gradient = gradients(
        block_inputs.reshape(TOKENS, WIDTH),
        mixed_inputs.reshape(TOKENS, WIDTH),
        head_weight,
        out_weight.reshape(WIDTH, WIDTH),
        final_gain,
        target_ids,
        token_ids,
    )
    shape = out_master.shape
    flat = (OWNED, WIDTH)
    results = adam(
        (
            (out_gradient, out_master.reshape(flat), out_first.reshape(flat), out_second.reshape(flat)),
            (head_gradient, head_master, head_first, head_second),
            (embed_gradient, embed_master, embed_first, embed_second),
        )
    )
    return (*(value.reshape(shape) for value in results[:3]), *results[3:])


def solution(mesh):
    tokens = P("section", None, "dp", None)
    rows = P("section", "dp", None)
    vocabulary = P(("section", "dp"), None)
    in_specs = (
        tokens, tokens, P(None, "dp"), P(None, "dp"), P(), P("section", None, None), P("section", None),
        rows, rows, rows, *(vocabulary,) * 6,
    )
    out_specs = (rows, rows, rows, *(vocabulary,) * 6)
    return jax.shard_map(
        per_device, mesh=mesh, in_specs=in_specs, out_specs=out_specs, check_vma=False
    )
```
